32 devices in a mesh: video: 4 (over z), span: 2 (over y), head: 4 (over x, core).
Axes of the slice: x: 2, y: 2, z: 4, core: 2. Of those that a mesh axis runs over, the one named last changes fastest.
Arguments:
- queries: bfloat16 [2048, 48, 128], P(('video', 'span', 'head')), parts along dimension 0, may hold values from -15 to 15
- key_rows: bfloat16 [2048, 48, 128], P(('video', 'span', 'head')), parts along dimension 0, may hold values from -6 to 6
- value_rows: bfloat16 [2048, 48, 128], P(('video', 'span', 'head')), parts along dimension 0, may hold values from -6 to 6
- noise_levels: int32 [8], P('video'), parts along dimension 0, may hold values from 0 to 7
- gate_table: float32 [8, 48], replicated, may hold values from 0.25 to 2
Outputs:
- attended: bfloat16 [2048, 48, 128], P(('video', 'span', 'head')), parts along dimension 0
The draws below stay inside these ranges and needn't reach their ends.
There are 4 independent parts, one for each index of `video`. The reference program is written for one: setup_inputs(seed, part) draws one part's arguments, and reference() takes and returns one part's arrays. A program takes and returns all parts, laid end to end along the dimension named above; an argument that names none is the same for every part. Nothing has to cross between parts.
All inputs are finite; a program needn't handle non-finite values.
Results may differ from the reference program's by a relative error of at most 0.0039.
Values may be sent and summed in bfloat16 or wider, within the bound.
No kernel may reach another device: no remote copies, remote signals or barrier semaphores. Data moves between devices by JAX's collectives and lax.ppermute only.
A program may use at most 128 MiB of HBM per device.

```python
import math
import jax
import jax.numpy as jnp
from jax import lax

HEADS = 48
HEAD_DIM = 128
BLOCK = 128
LEVELS = 8
CTOK = 256
SPANS = 2
TOKENS = 512
N_SPAN = 2


def draw_queries(key, part):
    noise_field = 2.5 * jax.random.truncated_normal(jax.random.fold_in(key, 1), -6.0, 6.0, (TOKENS, HEADS, HEAD_DIM), jnp.float32)
    return noise_field.astype(jnp.bfloat16)


def draw_key_rows(key, part):
    noise_field = jax.random.truncated_normal(jax.random.fold_in(key, 2), -6.0, 6.0, (TOKENS, HEADS, HEAD_DIM), jnp.float32)
    return noise_field.astype(jnp.bfloat16)


def level_of(stream_key, dims, split, low, top_value):
    loudness = 1.0
    for dim, parts in split:
        steps = jax.random.uniform(jax.random.fold_in(jax.random.fold_in(stream_key, 6), dim), (parts,), jnp.float32, low / len(split), top_value / len(split))
        loudness = loudness * jnp.repeat(jnp.exp(steps), dims[dim] // parts).reshape((-1,) + (1,) * (len(dims) - 1 - dim))
    return loudness


def noise(rng, shape, width, bound, cuts=(), kind=jnp.bfloat16):
    factor_of = level_of(rng, shape, cuts, -0.22, 0.18) if cuts else 1.0
    array = jax.random.normal(rng, shape, jnp.float32) * width * factor_of
    return jnp.minimum(jnp.maximum(array, -bound), bound).astype(kind)


def setup_inputs(seed: int = 0, part: int = 0) -> dict:
    seeds = jax.random.split(jax.random.key(seed), 6)
    part_keys = jax.random.split(jax.random.fold_in(seeds[5], part), 6)
    queries = draw_queries(jax.random.fold_in(jax.random.fold_in(seeds[5], part), 71), part)
    key_rows = draw_key_rows(jax.random.fold_in(jax.random.fold_in(seeds[5], part), 71), part)
    value_rows = noise(part_keys[2], (TOKENS, HEADS, HEAD_DIM), 1.0, 6.0, ((0, 8),))
    noise_levels = jax.random.randint(part_keys[3], (SPANS,), 0, LEVELS).astype(jnp.int32)
    gate_table = jnp.clip(jax.random.uniform(seeds[4], (LEVELS, HEADS), jnp.float32, 0.25, 2.0), 0.25, 2.0)
    return {"queries": queries, "key_rows": key_rows, "value_rows": value_rows, "noise_levels": noise_levels, "gate_table": gate_table}


def reference(queries, key_rows, value_rows, noise_levels, gate_table):
    score_scale = 1.0 / math.sqrt(HEAD_DIM)
    key_float = key_rows.astype(jnp.float32)
    value_float = value_rows.astype(jnp.float32)
    key_index = jnp.arange(TOKENS, dtype=jnp.int32)
    key_span = key_index // CTOK
    key_block = key_index % CTOK // BLOCK
    query_block = jnp.arange(CTOK, dtype=jnp.int32) // BLOCK

    def one_span(span_pos):
        first_row = (span_pos * CTOK).astype(jnp.int32)
        query_part = lax.dynamic_slice_in_dim(queries, first_row, CTOK, 0).astype(jnp.float32)
        scores = jnp.einsum('qhd,khd->qhk', query_part, key_float) * score_scale
        visible = (key_span[None, :] < span_pos) | (key_span[None, :] == span_pos) & (key_block[None, :] <= query_block[:, None])
        visible = visible[:, None, :]
        masked = jnp.where(visible, scores, -jnp.inf)
        row_max = lax.optimization_barrier(jnp.max(masked, axis=-1, keepdims=True))
        weights = jnp.where(visible, jnp.exp(masked - row_max), 0.0)
        totals = lax.optimization_barrier(jnp.sum(weights, axis=-1))
        rounded = lax.optimization_barrier(weights.astype(jnp.bfloat16))
        numerator = jnp.einsum('qhk,khd->qhd', rounded.astype(jnp.float32), value_float)
        one_hot = (jnp.arange(LEVELS, dtype=jnp.int32) == noise_levels[span_pos]).astype(jnp.float32)
        gate_row = jnp.dot(one_hot, gate_table, precision=lax.Precision.HIGHEST)
        result = numerator / totals[..., None] * gate_row[None, :, None]
        return result.astype(jnp.bfloat16)
    stacked = lax.map(one_span, jnp.arange(N_SPAN, dtype=jnp.int32))
    return stacked.reshape(TOKENS, HEADS, HEAD_DIM)
```

```python
import functools
import math

import jax
import jax.numpy as jnp
from jax import lax
from jax.experimental import pallas as pl
from jax.experimental.pallas import tpu as pltpu
from jax.sharding import PartitionSpec as P

BLOCK = 128
LEVELS = 8
TILE = 8


def from_behind(block, axis, distance):
    devices = range(lax.axis_size(axis))
    route = [(i - distance, i) for i in devices if i - distance in devices]
    return lax.ppermute(block, axis, route)


def gate_rows_for(noise_levels, gate_table):
    one_hot = (jnp.arange(LEVELS, dtype=jnp.int32)[None, :] == noise_levels[:, None]).astype(
        jnp.float32
    )
    return jnp.dot(one_hot, gate_table, precision=lax.Precision.HIGHEST)


def by_head(queries, key_rows, value_rows, noise_levels, gate_table):
    row_count, head_count, head_width = queries.shape
    head_groups = lax.axis_size("head")
    per_group = head_count // head_groups
    chain_len = lax.axis_size("span")
    chain_pos = lax.axis_index("span")
    score_scale = 1.0 / math.sqrt(head_width)
    split_shape = (row_count, head_groups, per_group, head_width)
    query_heads, key_heads, value_heads = (
        lax.all_to_all(
            queries.reshape(split_shape), "head", split_axis=1, concat_axis=0, tiled=True
        ),
        lax.all_to_all(
            key_rows.reshape(split_shape), "head", split_axis=1, concat_axis=0, tiled=True
        ),
        lax.all_to_all(
            value_rows.reshape(split_shape), "head", split_axis=1, concat_axis=0, tiled=True
        ),
    )
    span_len = row_count * head_groups
    query_heads = query_heads.reshape(span_len, per_group, head_width)
    key_heads = key_heads.reshape(span_len, per_group, head_width)
    value_heads = value_heads.reshape(span_len, per_group, head_width)
    own_scores = (
        jnp.einsum("qhd,khd->qhk", query_heads, key_heads, preferred_element_type=jnp.float32)
        * score_scale
    )
    query_block = jnp.arange(span_len, dtype=jnp.int32) // BLOCK
    visible = (query_block[None, :] <= query_block[:, None])[:, None, :]
    own_max = jnp.max(jnp.where(visible, own_scores, -jnp.inf), axis=-1)
    own_weights = jnp.where(visible, jnp.exp(own_scores - own_max[..., None]), 0.0)
    own_totals = jnp.sum(own_weights, axis=-1)
    own_acc = jnp.einsum(
        "qhk,khd->qhd",
        own_weights.astype(jnp.bfloat16),
        value_heads,
        preferred_element_type=jnp.float32,
    )
    running = (own_max, own_totals, own_acc)

    def update(state_now, key_block, value_block):
        row_max, totals, accum = state_now
        scores = (
            jnp.einsum("qhd,khd->qhk", query_heads, key_block, preferred_element_type=jnp.float32)
            * score_scale
        )
        new_max = jnp.maximum(row_max, jnp.max(scores, axis=-1))
        rescale = jnp.exp(row_max - new_max)
        weights = jnp.exp(scores - new_max[..., None])
        totals = totals * rescale + jnp.sum(weights, axis=-1)
        accum = accum * rescale[..., None] + jnp.einsum(
            "qhk,khd->qhd",
            weights.astype(jnp.bfloat16),
            value_block,
            preferred_element_type=jnp.float32,
        )
        return (new_max, totals, accum)

    def advance(state_now, inputs):
        key_block, value_block, span_id = inputs
        useful = (span_id >= 0) & (span_id < chain_pos)
        return (
            lax.cond(
                useful,
                lambda inner: update(inner, key_block, value_block),
                lambda inner: inner,
                state_now,
            ),
            None,
        )

    def relay_turn(turn, loop_state):
        state_now, in_hand = loop_state
        in_hand = from_behind(in_hand, "span", 1)
        state_now, unused = advance(state_now, (in_hand[0], in_hand[1], chain_pos - 1 - turn))
        return (state_now, in_hand)

    running, in_hand = lax.fori_loop(
        0, chain_len - 1, relay_turn, (running, jnp.stack((key_heads, value_heads)))
    )
    row_max, totals, accum = running
    gate_rows = gate_rows_for(noise_levels, gate_table)
    gate_row = lax.dynamic_index_in_dim(gate_rows, chain_pos, 0, keepdims=False)
    my_gates = lax.dynamic_slice_in_dim(gate_row, lax.axis_index("head") * per_group, per_group, 0)
    result = (accum / totals[..., None] * my_gates[None, :, None]).astype(jnp.bfloat16)
    returned = lax.all_to_all(
        result.reshape(span_len, 1, per_group, head_width),
        "head",
        split_axis=0,
        concat_axis=1,
        tiled=True,
    )
    return returned.reshape(row_count, head_count, head_width)


def score_factor(width):
    return math.log2(math.e) / math.sqrt(width)


def partial_softmax(query, keys, values, shifts, factor):
    scores = [
        lax.dot_general(query, k, (((1,), (1,)), ((), ())), preferred_element_type=jnp.float32)
        for k in keys
    ]
    scores = [s if b is None else s + b for s, b in zip(scores, shifts)]
    top = functools.reduce(jnp.maximum, [jnp.max(s, axis=1, keepdims=True) for s in scores])
    weights = [jnp.exp2((s - top) * factor) for s in scores]
    total = sum(jnp.sum(w, axis=1, keepdims=True) for w in weights)
    summed = sum(
        lax.dot_general(
            w.astype(jnp.bfloat16), v, (((1,), (0,)), ((), ())), preferred_element_type=jnp.float32
        )
        for w, v in zip(weights, values)
    )
    return summed / total, top * factor + jnp.log2(total)


def both(a, b):
    return jnp.concatenate([a, b], axis=0)


def attend_kernel(heads, factor, two, flags, *refs):
    if two:
        q, k0, k1, v0, v1, rk0, rk1, rv0, rv1 = refs[:9]
    else:
        q, k0, k1, v0, v1 = refs[:5]
    out, weight = refs[-2:]
    step = pl.program_id(0)
    rows, width = q.shape[1:]
    lane = lax.broadcasted_iota(jnp.int32, (rows, width), 1)

    @pl.when(step == 0)
    def _():
        weight[...] = jnp.zeros_like(weight)

    own_shift = jnp.where(flags[1] == 1, 0.0, -jnp.inf)
    received_shift = jnp.where(flags[2] == 1, 0.0, -jnp.inf)
    found = weight[0]
    for h in range(heads):
        keys, values, shifts = [both(k0[h], k1[h])], [both(v0[h], v1[h])], [None]
        if two:
            keys.append(both(rk0[h], rk1[h]))
            values.append(both(rv0[h], rv1[h]))
            shifts = [own_shift, received_shift]
        part, log_weight = partial_softmax(q[h], keys, values, shifts, factor)
        out[h] = part.astype(out.dtype)
        found = jnp.where(lane == step * heads + h, log_weight, found)
    weight[0] = found


def attend(flags, group, queries, query_group, own, received, dtype, into=None):
    per_group, rows, width = own[0].shape
    per_group //= 2
    steps = per_group // TILE

    def block(at_group):
        return pl.BlockSpec(
            (TILE, rows, width),
            (lambda i, f, g=at_group: (f[g] * steps + i, 0, 0)) if at_group is not None else (lambda i, f: (i, 0, 0)),
        )

    two = received is not None
    operands = [queries, *own]
    specs = [block(query_group)] + [block(group)] * 4
    if two:
        operands += list(received)
        specs += [block(None)] * 4
    if into is None:
        out_shape = (
            jax.ShapeDtypeStruct((per_group, rows, width), dtype),
            jax.ShapeDtypeStruct((1, rows, width), jnp.float32),
        )
        out_specs = (block(None), pl.BlockSpec((1, rows, width), lambda i, f: (0, 0, 0)))
        aliases = {}
    else:
        out_shape = (
            jax.ShapeDtypeStruct((2 * per_group, rows, width), dtype),
            jax.ShapeDtypeStruct((2, rows, width), jnp.float32),
        )
        out_specs = (block(group), pl.BlockSpec((1, rows, width), lambda i, f: (f[group], 0, 0)))
        aliases = {}
        if into != ():
            aliases = {1 + len(operands): 0, 2 + len(operands): 1}
            operands += list(into)
            specs += [pl.BlockSpec(memory_space=pl.ANY)] * 2
    pairs = 2 if two else 1
    work = per_group * rows * 2 * rows * width * 4 * pairs
    return pl.pallas_call(
        functools.partial(attend_kernel, TILE, score_factor(width), two),
        out_shape=out_shape,
        grid_spec=pltpu.PrefetchScalarGridSpec(
            num_scalar_prefetch=1, grid=(steps,), in_specs=specs, out_specs=out_specs
        ),
        input_output_aliases=aliases,
        cost_estimate=pl.CostEstimate(
            flops=work * 10, bytes_accessed=sum(o.size * 2 for o in operands), transcendentals=work // width // 4
        ),
    )(flags, *operands)


def merge_kernel(
    heads, per_group, factor, flags, gates, local, local_weight, upper, upper_weight, across, across_weight,
    extra, extra_weight, q, k0, k1, v0, v1, out, scratch,
):
    step = pl.program_id(0)
    steps = per_group // heads
    group = step // steps
    first = step * heads - group * per_group
    rows, width = q.shape[1:]
    lane = lax.broadcasted_iota(jnp.int32, (rows, width), 1)
    no = -jnp.inf
    later = flags[0] == 1

    def column(table, h):
        return jnp.sum(jnp.where(lane == first + h, table, 0.0), axis=1, keepdims=True)

    def finish(parts, h):
        top = functools.reduce(jnp.maximum, [w for _, w in parts])
        scaled = [jnp.exp2(w - top) for _, w in parts]
        summed = sum(p.astype(jnp.float32) * s for (p, _), s in zip(parts, scaled))
        scratch[h] = summed * (gates[step * heads + h] / sum(scaled))

    @pl.when(group == 0)
    def _():
        upper_shift = jnp.where(later, 0.0, no)
        extra_shift = jnp.where(flags[3] == 1, 0.0, no)
        for h in range(heads):
            finish(
                [
                    (local[h], column(local_weight[0], h)),
                    (upper[h], column(upper_weight[0], h) + upper_shift),
                    (extra[h], column(extra_weight[0], h) + extra_shift),
                ],
                h,
            )

    @pl.when((group == 1) & later)
    def _():
        for h in range(heads):
            finish([(local[h], column(local_weight[0], h)), (across[h], column(across_weight[0], h))], h)

    @pl.when((group == 1) & jnp.logical_not(later) & (flags[2] == 0))
    def _():
        for h in range(heads):
            scratch[h] = local[h] * gates[step * heads + h]

    @pl.when((group == 1) & jnp.logical_not(later) & (flags[2] == 1))
    def _():
        for h in range(heads):
            part, weight = partial_softmax(
                q[h], [both(k0[h], k1[h])], [both(v0[h], v1[h])], [None], factor
            )
            finish([(local[h], column(local_weight[0], h)), (part, weight)], h)

    out[...] = jnp.swapaxes(scratch[...], 0, 1).astype(out.dtype)


def merge(flags, gates, local, upper, across, extra, queries, received):
    heads, rows, width = local[0].shape
    per_group = heads // 2
    steps = per_group // TILE
    whole = pl.BlockSpec((TILE, rows, width), lambda i, f, g: (i, 0, 0))
    in_a = pl.BlockSpec((TILE, rows, width), lambda i, f, g: (jnp.minimum(i, steps - 1), 0, 0))
    in_b = pl.BlockSpec((TILE, rows, width), lambda i, f, g: (jnp.maximum(i - steps, 0), 0, 0))
    one = pl.BlockSpec((1, rows, width), lambda i, f, g: (0, 0, 0))
    return pl.pallas_call(
        functools.partial(merge_kernel, TILE, per_group, score_factor(width)),
        out_shape=jax.ShapeDtypeStruct((rows, heads, width), jnp.bfloat16),
        grid_spec=pltpu.PrefetchScalarGridSpec(
            num_scalar_prefetch=2,
            grid=(2 * steps,),
            in_specs=[
                whole, pl.BlockSpec((1, rows, width), lambda i, f, g: (i // steps, 0, 0)),
                in_a, one, in_b, one, in_a, one, whole, in_b, in_b, in_b, in_b,
            ],
            out_specs=pl.BlockSpec((rows, TILE, width), lambda i, f, g: (0, i, 0)),
            scratch_shapes=[pltpu.VMEM((TILE, rows, width), jnp.float32)],
        ),
    )(flags, gates, *local, *upper, *across, *extra, queries, *received)


def by_block(queries, key_rows, value_rows, noise_levels, gate_table):
    rows, heads, width = queries.shape
    half = heads // 2
    per_span = lax.axis_size("head")
    share = per_span // 2
    span, place = lax.axis_index("span"), lax.axis_index("head")
    side = place // share
    later = span == 1
    devices = range(2 * per_span)

    def send(block, target):
        route = [(p, target(p)) for p in devices if target(p) is not None]
        return lax.ppermute(block, ("span", "head"), route)

    def sideways(p):
        return p ^ share

    def other_span(p):
        return p ^ per_span

    def up(p):
        return p + per_span if p < per_span else None

    def partner(p):
        return p ^ 1

    def in_block(p, number):
        return p // share == number

    q, k, v = (jnp.transpose(a, (1, 0, 2)) for a in (queries, key_rows, value_rows))
    first = slice(0, half)
    second = slice(half, heads)

    x1 = send(jnp.where(later, q[second], k[first]), sideways)
    y1 = send(jnp.where(later, q[first], k[second]), other_span)
    x2 = send(
        jnp.where(later, q[first], v[first]), lambda p: None if in_block(p, 2) else sideways(p)
    )
    y2 = send(v[second], up)
    own_k1, own_v1 = send(k, partner), send(v, partner)
    x3, x4 = (send(a[second], lambda p: sideways(p) if in_block(p, 0) else None) for a in (k, v))

    gate_rows = gate_rows_for(noise_levels, gate_table)
    gates = lax.dynamic_index_in_dim(gate_rows, span, 0, keepdims=False)

    one = jnp.int32(1)
    block_number = 2 * span + side
    def flags_of(own, received):
        return jnp.stack(
            [span, own, received, (block_number == 3).astype(jnp.int32), 1 - span, 0 * span]
        ).astype(jnp.int32)

    own = (k, own_k1, v, own_v1)
    plain = flags_of(one, one)
    local = attend(plain, 4, q, 4, own, None, jnp.float32, into=())
    visitor = jnp.where(later, x1, y1)
    got_k, got_v = jnp.where(later, y1, x1), jnp.where(later, y2, x2)
    received = (got_k, send(got_k, partner), got_v, send(got_v, partner))
    extra = attend(plain, 5, x2, None, own, None, jnp.bfloat16)
    away = attend(
        flags_of((block_number != 3).astype(jnp.int32), one), 0, visitor, None, own, received, jnp.bfloat16
    )
    upper = [send(a, up) for a in away]
    across = [send(a, lambda p: sideways(p) if p >= per_span else None) for a in away]
    extra = [send(a, lambda p: sideways(p) if in_block(p, 2) else None) for a in extra]
    local = attend(
        flags_of(one, (block_number != 0).astype(jnp.int32)), 0, q, 0, own, received, jnp.float32, into=local
    )
    late_k1, late_v1 = (
        send(a, lambda p: partner(p) if in_block(p, 1) else None) for a in (x3, x4)
    )
    return merge(
        flags_of(one, (block_number == 1).astype(jnp.int32)),
        gates, local, upper, across, extra, q, (x3, late_k1, x4, late_v1),
    )


def body(queries, key_rows, value_rows, noise_levels, gate_table):
    rows, heads, _ = queries.shape
    spans, per_span = lax.axis_size("span"), lax.axis_size("head")
    two_by_two = spans == 2 and 2 * rows == BLOCK and per_span * rows == 2 * BLOCK
    if two_by_two and heads % (2 * TILE) == 0:
        return by_block(queries, key_rows, value_rows, noise_levels, gate_table)
    return by_head(queries, key_rows, value_rows, noise_levels, gate_table)


def solution(mesh):
    tokens = ("video", "span", "head")
    return jax.shard_map(
        body,
        mesh=mesh,
        in_specs=(
            P(tokens, None, None),
            P(tokens, None, None),
            P(tokens, None, None),
            P("video"),
            P(),
        ),
        out_specs=P(tokens, None, None),
        check_vma=False,
    )
```

```python
import functools
import math

import jax
import jax.numpy as jnp
from jax import lax
from jax.experimental import pallas as pl
from jax.experimental.pallas import tpu as pltpu
from jax.sharding import PartitionSpec as P

BLOCK = 128
LEVELS = 8
TILE = 8
LANES = 32


def from_behind(block, axis, distance):
    devices = range(lax.axis_size(axis))
    route = [(i - distance, i) for i in devices if i - distance in devices]
    return lax.ppermute(block, axis, route)


def gate_rows_for(noise_levels, gate_table):
    one_hot = (jnp.arange(LEVELS, dtype=jnp.int32)[None, :] == noise_levels[:, None]).astype(
        jnp.float32
    )
    return jnp.dot(one_hot, gate_table, precision=lax.Precision.HIGHEST)


def by_head(queries, key_rows, value_rows, noise_levels, gate_table):
    row_count, head_count, head_width = queries.shape
    head_groups = lax.axis_size("head")
    per_group = head_count // head_groups
    chain_len = lax.axis_size("span")
    chain_pos = lax.axis_index("span")
    score_scale = 1.0 / math.sqrt(head_width)
    split_shape = (row_count, head_groups, per_group, head_width)
    query_heads, key_heads, value_heads = (
        lax.all_to_all(
            queries.reshape(split_shape), "head", split_axis=1, concat_axis=0, tiled=True
        ),
        lax.all_to_all(
            key_rows.reshape(split_shape), "head", split_axis=1, concat_axis=0, tiled=True
        ),
        lax.all_to_all(
            value_rows.reshape(split_shape), "head", split_axis=1, concat_axis=0, tiled=True
        ),
    )
    span_len = row_count * head_groups
    query_heads = query_heads.reshape(span_len, per_group, head_width)
    key_heads = key_heads.reshape(span_len, per_group, head_width)
    value_heads = value_heads.reshape(span_len, per_group, head_width)
    own_scores = (
        jnp.einsum("qhd,khd->qhk", query_heads, key_heads, preferred_element_type=jnp.float32)
        * score_scale
    )
    query_block = jnp.arange(span_len, dtype=jnp.int32) // BLOCK
    visible = (query_block[None, :] <= query_block[:, None])[:, None, :]
    own_max = jnp.max(jnp.where(visible, own_scores, -jnp.inf), axis=-1)
    own_weights = jnp.where(visible, jnp.exp(own_scores - own_max[..., None]), 0.0)
    own_totals = jnp.sum(own_weights, axis=-1)
    own_acc = jnp.einsum(
        "qhk,khd->qhd",
        own_weights.astype(jnp.bfloat16),
        value_heads,
        preferred_element_type=jnp.float32,
    )
    running = (own_max, own_totals, own_acc)

    def update(state_now, key_block, value_block):
        row_max, totals, accum = state_now
        scores = (
            jnp.einsum("qhd,khd->qhk", query_heads, key_block, preferred_element_type=jnp.float32)
            * score_scale
        )
        new_max = jnp.maximum(row_max, jnp.max(scores, axis=-1))
        rescale = jnp.exp(row_max - new_max)
        weights = jnp.exp(scores - new_max[..., None])
        totals = totals * rescale + jnp.sum(weights, axis=-1)
        accum = accum * rescale[..., None] + jnp.einsum(
            "qhk,khd->qhd",
            weights.astype(jnp.bfloat16),
            value_block,
            preferred_element_type=jnp.float32,
        )
        return (new_max, totals, accum)

    def advance(state_now, inputs):
        key_block, value_block, span_id = inputs
        useful = (span_id >= 0) & (span_id < chain_pos)
        return (
            lax.cond(
                useful,
                lambda inner: update(inner, key_block, value_block),
                lambda inner: inner,
                state_now,
            ),
            None,
        )

    def relay_turn(turn, loop_state):
        state_now, in_hand = loop_state
        in_hand = from_behind(in_hand, "span", 1)
        state_now, _ = advance(state_now, (in_hand[0], in_hand[1], chain_pos - 1 - turn))
        return (state_now, in_hand)

    running, _ = lax.fori_loop(
        0, chain_len - 1, relay_turn, (running, jnp.stack((key_heads, value_heads)))
    )
    _, totals, accum = running
    gate_rows = gate_rows_for(noise_levels, gate_table)
    gate_row = lax.dynamic_index_in_dim(gate_rows, chain_pos, 0, keepdims=False)
    my_gates = lax.dynamic_slice_in_dim(gate_row, lax.axis_index("head") * per_group, per_group, 0)
    result = (accum / totals[..., None] * my_gates[None, :, None]).astype(jnp.bfloat16)
    returned = lax.all_to_all(
        result.reshape(span_len, 1, per_group, head_width),
        "head",
        split_axis=0,
        concat_axis=1,
        tiled=True,
    )
    return returned.reshape(row_count, head_count, head_width)


def attend(jobs, factor):
    scores = [
        [lax.dot_general(q, k, (((1,), (1,)), ((), ())), preferred_element_type=jnp.float32) for k in keys]
        for q, keys, _, _ in jobs
    ]
    scores = [
        [s if shift is None else s + shift for s, shift in zip(of_head, job[3])]
        for of_head, job in zip(scores, jobs)
    ]
    tops = [
        functools.reduce(jnp.maximum, [jnp.max(s, axis=1, keepdims=True) for s in of_head])
        for of_head in scores
    ]
    weights = [[jnp.exp2((s - top) * factor) for s in of_head] for of_head, top in zip(scores, tops)]
    totals = [sum(jnp.sum(w, axis=1, keepdims=True) for w in of_head) for of_head in weights]
    sums = [
        sum(
            lax.dot_general(
                w.astype(jnp.bfloat16), v, (((1,), (0,)), ((), ())), preferred_element_type=jnp.float32
            )
            for w, v in zip(of_head, job[2])
        )
        for of_head, job in zip(weights, jobs)
    ]
    return (
        [s * (1.0 / t) for s, t in zip(sums, totals)],
        [top * factor + jnp.log2(t) for top, t in zip(tops, totals)],
    )


def lanes_of(rows, width):
    return lax.broadcasted_iota(jnp.int32, (rows, width), 1)


def table_of(columns, lane):
    table = jnp.zeros(lane.shape, jnp.float32)
    for h, column in enumerate(columns):
        table = jnp.where(lane % LANES == h, column, table)
    return table


def split_table(table, lane):
    high = table.astype(jnp.bfloat16).astype(jnp.float32)
    rest = table - high
    middle = rest.astype(jnp.bfloat16).astype(jnp.float32)
    parts = jnp.where(lane < LANES, high, jnp.where(lane < 2 * LANES, middle, rest - middle))
    return jnp.where(lane < 3 * LANES, parts, 0.0).astype(jnp.bfloat16)


def column_of(table, chosen):
    return jnp.sum(jnp.where(chosen, table.astype(jnp.float32), 0.0), axis=1, keepdims=True)


def both(pair, h):
    return jnp.concatenate([pair[0][h], pair[1][h]], axis=0)


def store(out, parts, log_weights, lane):
    for h, part in enumerate(parts):
        out[h] = part.astype(out.dtype)
    out[len(parts)] = split_table(table_of(log_weights, lane), lane)


def store_local(out, table, parts, log_weights, lane):
    for h, part in enumerate(parts):
        out[h] = part
    table[...] = table_of(log_weights, lane)


def where_am_i():
    span = lax.axis_index("span")
    return span, 2 * span + lax.axis_index("head") // 2


def unless(seen):
    return jnp.where(seen, 0.0, -jnp.inf)


def own_kernel(factor, q, k0, k1, v0, v1, out, table):
    span, _ = where_am_i()
    rows, width = q.shape[1:]
    half = out.shape[0]
    first = (1 - span) * half
    jobs = [
        (q[first + h], [both((k0, k1), first + h)], [both((v0, v1), first + h)], [None])
        for h in range(half)
    ]
    store_local(out, table, *attend(jobs, factor), lanes_of(rows, width))


def visit_kernel(factor, q, rk0, rk1, rv0, rv1, k0, k1, v0, v1, out):
    span, block = where_am_i()
    half, rows, width = q.shape
    first = span * half
    shift = unless(block != 3)
    jobs = [
        (
            q[h],
            [both((rk0, rk1), h), both((k0, k1), first + h)],
            [both((rv0, rv1), h), both((v0, v1), first + h)],
            [None, shift],
        )
        for h in range(half)
    ]
    store(out, *attend(jobs, factor), lanes_of(rows, width))


def stay_kernel(factor, q, rk0, rk1, rv0, rv1, k0, k1, v0, v1, out, table):
    span, block = where_am_i()
    rows, width = q.shape[1:]
    half = out.shape[0]
    first = span * half
    shift = unless(block != 0)
    jobs = [
        (
            q[first + h],
            [both((k0, k1), first + h), both((rk0, rk1), h)],
            [both((v0, v1), first + h), both((rv0, rv1), h)],
            [None, shift],
        )
        for h in range(half)
    ]
    store_local(out, table, *attend(jobs, factor), lanes_of(rows, width))


def guest_kernel(factor, host, first, q, k0, k1, v0, v1, out):
    _, block = where_am_i()
    heads, rows, width = q.shape

    @pl.when(block == host)
    def _():
        jobs = [
            (q[h], [both((k0, k1), first + h)], [both((v0, v1), first + h)], [None])
            for h in range(heads)
        ]
        store(out, *attend(jobs, factor), lanes_of(rows, width))


def fetched_kernel(factor, host, first, q, k0, k1, v0, v1, out, table):
    _, block = where_am_i()
    heads, rows, width = out.shape

    @pl.when(block == host)
    def _():
        jobs = [
            (q[first + h], [both((k0, k1), h)], [both((v0, v1), h)], [None]) for h in range(heads)
        ]
        store_local(out, table, *attend(jobs, factor), lanes_of(rows, width))


def merge_kernel(
    levels, gate_table, other, other_table, mine, mine_table, upper, across, extra, lent, fetched, fetched_table, out
):
    span, block = where_am_i()
    half, rows, width = mine.shape
    part_heads = fetched.shape[0]
    lane = lanes_of(rows, width)
    level = levels[span]

    def finish(first, parts_of):
        for start in range(0, half, TILE):
            heads = range(start, start + TILE)
            parts = [parts_of(h) for h in heads]
            tops = [functools.reduce(jnp.maximum, [w for _, w in of_head]) for of_head in parts]
            scaled = [
                [jnp.exp2(w - top) for _, w in of_head] for of_head, top in zip(parts, tops)
            ]
            factors = [gate_table[level, first + h] / sum(s) for h, s in zip(heads, scaled)]
            sums = [
                sum(p.astype(jnp.float32) * (s * f) for (p, _), s in zip(of_head, of_scale))
                for of_head, of_scale, f in zip(parts, scaled, factors)
            ]
            together = jnp.swapaxes(jnp.stack(sums), 0, 1)
            out[:, first + start : first + start + TILE, :] = together.astype(out.dtype)

    def sent(slab, h, shift=0.0):
        return slab[h], column_of(slab[slab.shape[0] - 1], lane % LANES == h) + shift

    def kept(parts, table, h):
        return parts[h], column_of(table[...], lane == h)

    @pl.when(span == 1)
    def _():
        shift = unless(block == 3)
        finish(0, lambda h: [kept(other, other_table, h), sent(upper, h), sent(extra, h, shift)])
        finish(half, lambda h: [kept(mine, mine_table, h), sent(across, h)])

    @pl.when(block == 0)
    def _():
        finish(0, lambda h: [kept(mine, mine_table, h)])
        finish(half, lambda h: [kept(other, other_table, h)])

    @pl.when(block == 1)
    def _():
        finish(0, lambda h: [kept(mine, mine_table, h)])
        lent_heads = half - part_heads
        finish(
            half,
            lambda h: [
                kept(other, other_table, h),
                sent(lent, h) if h < lent_heads else kept(fetched, fetched_table, h - lent_heads),
            ],
        )


def run(kernel, out_shape, operands, scalars=()):
    in_vmem, in_smem = pl.BlockSpec(memory_space=pltpu.VMEM), pl.BlockSpec(memory_space=pltpu.SMEM)
    return pl.pallas_call(
        kernel,
        out_shape=out_shape,
        in_specs=[in_smem] * len(scalars) + [in_vmem] * len(operands),
        out_specs=jax.tree.map(lambda _: in_vmem, out_shape),
        compiler_params=pltpu.CompilerParams(vmem_limit_bytes=8 << 20),
        cost_estimate=pl.CostEstimate(flops=2_000_000_000, bytes_accessed=1 << 20, transcendentals=0),
    )(*scalars, *operands)


def by_block(queries, key_rows, value_rows, noise_levels, gate_table):
    rows, heads, width = queries.shape
    half = heads // 2
    lent = half // 2
    per_span = lax.axis_size("head")
    share = per_span // 2
    span, side = lax.axis_index("span"), lax.axis_index("head") // share
    later = span == 1
    factor = math.log2(math.e) / math.sqrt(width)
    devices = range(2 * per_span)

    def send(block, target):
        route = [(p, target(p)) for p in devices if target(p) is not None]
        return lax.ppermute(block, ("span", "head"), route)

    def sideways(p):
        return p ^ share

    def other_span(p):
        return p ^ per_span

    def partner(p):
        return p ^ 1

    def only(numbers, target):
        return lambda p: target(p) if p // share in numbers else None

    def up(p):
        return p + per_span if p < per_span else None

    def moved(block, target):
        return send(block, target)

    def by_head_first(a):
        return jnp.transpose(a, (1, 0, 2))

    x1 = by_head_first(jnp.where(later, queries[:, :half], key_rows[:, :half]))
    y1 = by_head_first(jnp.where(later, queries[:, :half], key_rows[:, half:]))
    x1, y1, *raw = lax.optimization_barrier((x1, y1, queries, key_rows, value_rows))
    q, k, v = map(by_head_first, raw)
    x1 = moved(x1, only((0, 1, 3), sideways))
    y1 = moved(y1, other_span)
    own_k, own_v = moved(k, partner), moved(v, partner)
    x2 = moved(jnp.where(later, q[half:], v[:half]), sideways)
    y2 = moved(v[half:], other_span)
    x3 = moved(jnp.where(side == 0, k[half + lent :], q[half : half + lent]), only((0, 1), sideways))
    x4 = moved(v[half + lent :], only((0,), sideways))

    def slab(n):
        return jax.ShapeDtypeStruct((n + 1, rows, width), jnp.bfloat16)

    def kept(n):
        return (
            jax.ShapeDtypeStruct((n, rows, width), jnp.float32),
            jax.ShapeDtypeStruct((rows, width), jnp.float32),
        )

    def kernel(body, out_shape, *operands):
        return run(body, out_shape, operands)

    own = (k, own_k, v, own_v)
    other = kernel(functools.partial(own_kernel, factor), kept(half), q, *own)
    extra = kernel(functools.partial(guest_kernel, factor, 2, 0), slab(half), x1, *own)
    extra = moved(extra, only((2,), sideways))

    got_k = jnp.where(later, y1, x1)
    got_k1 = moved(got_k, partner)
    visitor, got_v = jnp.where(later, x2, y1), jnp.where(later, y2, x2)
    got_v1 = moved(got_v, partner)
    received = (got_k, got_k1, got_v, got_v1)
    away = kernel(functools.partial(visit_kernel, factor), slab(half), visitor, *received, *own)
    upper = moved(away, up)
    across = moved(away, only((2, 3), sideways))
    mine = kernel(functools.partial(stay_kernel, factor), kept(half), q, *received, *own)

    helped = kernel(functools.partial(guest_kernel, factor, 0, half), slab(lent), x3, *own)
    helped = moved(helped, only((0,), sideways))
    x3_1, x4_1 = (moved(a, only((1,), partner)) for a in (x3, x4))
    fetched = kernel(
        functools.partial(fetched_kernel, factor, 1, half + lent), kept(half - lent), q, x3, x3_1, x4, x4_1
    )
    return run(
        merge_kernel,
        jax.ShapeDtypeStruct((rows, heads, width), jnp.bfloat16),
        (*other, *mine, upper, across, extra, helped, *fetched),
        (noise_levels, gate_table),
    )


def body(queries, key_rows, value_rows, noise_levels, gate_table):
    rows, heads, _ = queries.shape
    spans, per_span = lax.axis_size("span"), lax.axis_size("head")
    two_by_two = spans == 2 and 2 * rows == BLOCK and per_span * rows == 2 * BLOCK
    if two_by_two and heads % (2 * TILE) == 0 and heads <= 2 * LANES:
        return by_block(queries, key_rows, value_rows, noise_levels, gate_table)
    return by_head(queries, key_rows, value_rows, noise_levels, gate_table)


def solution(mesh):
    tokens = ("video", "span", "head")
    return jax.shard_map(
        body,
        mesh=mesh,
        in_specs=(
            P(tokens, None, None),
            P(tokens, None, None),
            P(tokens, None, None),
            P("video"),
            P(),
        ),
        out_specs=P(tokens, None, None),
        check_vma=False,
    )
```

```python
import functools
import math

import jax
import jax.numpy as jnp
from jax import lax
from jax.experimental import pallas as pl
from jax.experimental.pallas import tpu as pltpu
from jax.sharding import PartitionSpec as P

BLOCK = 128
LEVELS = 8
TILE = 8
LANES = 32


def from_behind(block, axis, distance):
    devices = range(lax.axis_size(axis))
    route = [(i - distance, i) for i in devices if i - distance in devices]
    return lax.ppermute(block, axis, route)


def gate_rows_for(noise_levels, gate_table):
    one_hot = (jnp.arange(LEVELS, dtype=jnp.int32)[None, :] == noise_levels[:, None]).astype(
        jnp.float32
    )
    return jnp.dot(one_hot, gate_table, precision=lax.Precision.HIGHEST)


def by_head(queries, key_rows, value_rows, noise_levels, gate_table):
    row_count, head_count, head_width = queries.shape
    head_groups = lax.axis_size("head")
    per_group = head_count // head_groups
    chain_len = lax.axis_size("span")
    chain_pos = lax.axis_index("span")
    score_scale = 1.0 / math.sqrt(head_width)
    split_shape = (row_count, head_groups, per_group, head_width)
    query_heads, key_heads, value_heads = (
        lax.all_to_all(
            queries.reshape(split_shape), "head", split_axis=1, concat_axis=0, tiled=True
        ),
        lax.all_to_all(
            key_rows.reshape(split_shape), "head", split_axis=1, concat_axis=0, tiled=True
        ),
        lax.all_to_all(
            value_rows.reshape(split_shape), "head", split_axis=1, concat_axis=0, tiled=True
        ),
    )
    span_len = row_count * head_groups
    query_heads = query_heads.reshape(span_len, per_group, head_width)
    key_heads = key_heads.reshape(span_len, per_group, head_width)
    value_heads = value_heads.reshape(span_len, per_group, head_width)
    own_scores = (
        jnp.einsum("qhd,khd->qhk", query_heads, key_heads, preferred_element_type=jnp.float32)
        * score_scale
    )
    query_block = jnp.arange(span_len, dtype=jnp.int32) // BLOCK
    visible = (query_block[None, :] <= query_block[:, None])[:, None, :]
    own_max = jnp.max(jnp.where(visible, own_scores, -jnp.inf), axis=-1)
    own_weights = jnp.where(visible, jnp.exp(own_scores - own_max[..., None]), 0.0)
    own_totals = jnp.sum(own_weights, axis=-1)
    own_acc = jnp.einsum(
        "qhk,khd->qhd",
        own_weights.astype(jnp.bfloat16),
        value_heads,
        preferred_element_type=jnp.float32,
    )
    running = (own_max, own_totals, own_acc)

    def update(state_now, key_block, value_block):
        row_max, totals, accum = state_now
        scores = (
            jnp.einsum("qhd,khd->qhk", query_heads, key_block, preferred_element_type=jnp.float32)
            * score_scale
        )
        new_max = jnp.maximum(row_max, jnp.max(scores, axis=-1))
        rescale = jnp.exp(row_max - new_max)
        weights = jnp.exp(scores - new_max[..., None])
        totals = totals * rescale + jnp.sum(weights, axis=-1)
        accum = accum * rescale[..., None] + jnp.einsum(
            "qhk,khd->qhd",
            weights.astype(jnp.bfloat16),
            value_block,
            preferred_element_type=jnp.float32,
        )
        return (new_max, totals, accum)

    def advance(state_now, inputs):
        key_block, value_block, span_id = inputs
        useful = (span_id >= 0) & (span_id < chain_pos)
        return (
            lax.cond(
                useful,
                lambda inner: update(inner, key_block, value_block),
                lambda inner: inner,
                state_now,
            ),
            None,
        )

    def relay_turn(turn, loop_state):
        state_now, in_hand = loop_state
        in_hand = from_behind(in_hand, "span", 1)
        state_now, _ = advance(state_now, (in_hand[0], in_hand[1], chain_pos - 1 - turn))
        return (state_now, in_hand)

    running, _ = lax.fori_loop(
        0, chain_len - 1, relay_turn, (running, jnp.stack((key_heads, value_heads)))
    )
    _, totals, accum = running
    gate_rows = gate_rows_for(noise_levels, gate_table)
    gate_row = lax.dynamic_index_in_dim(gate_rows, chain_pos, 0, keepdims=False)
    my_gates = lax.dynamic_slice_in_dim(gate_row, lax.axis_index("head") * per_group, per_group, 0)
    result = (accum / totals[..., None] * my_gates[None, :, None]).astype(jnp.bfloat16)
    returned = lax.all_to_all(
        result.reshape(span_len, 1, per_group, head_width),
        "head",
        split_axis=0,
        concat_axis=1,
        tiled=True,
    )
    return returned.reshape(row_count, head_count, head_width)


def attend(jobs, factor, shift=None):
    scores = [
        lax.dot_general(q, k, (((1,), (1,)), ((), ())), preferred_element_type=jnp.float32)
        for q, k, _ in jobs
    ]
    if shift is not None:
        scores = [s + shift for s in scores]
    tops = [jnp.max(s, axis=1, keepdims=True) for s in scores]
    weights = [jnp.exp2((s - top) * factor) for s, top in zip(scores, tops)]
    totals = [jnp.sum(w, axis=1, keepdims=True) for w in weights]
    sums = [
        lax.dot_general(
            w.astype(jnp.bfloat16), v, (((1,), (0,)), ((), ())), preferred_element_type=jnp.float32
        )
        for w, (_, _, v) in zip(weights, jobs)
    ]
    return (
        [s * (1.0 / t) for s, t in zip(sums, totals)],
        [top * factor + jnp.log2(t) for top, t in zip(tops, totals)],
    )


def lanes_of(rows, width):
    return lax.broadcasted_iota(jnp.int32, (rows, width), 1)


def table_of(columns, lane):
    table = jnp.zeros(lane.shape, jnp.float32)
    for h, column in enumerate(columns):
        table = jnp.where(lane % LANES == h, column, table)
    return table


def split_table(table, lane):
    high = table.astype(jnp.bfloat16).astype(jnp.float32)
    rest = table - high
    middle = rest.astype(jnp.bfloat16).astype(jnp.float32)
    parts = jnp.where(lane < LANES, high, jnp.where(lane < 2 * LANES, middle, rest - middle))
    return jnp.where(lane < 3 * LANES, parts, 0.0).astype(jnp.bfloat16)


def joined(table):
    parts = table.astype(jnp.float32)
    return parts + pltpu.roll(parts, parts.shape[1] - LANES, 1) + pltpu.roll(parts, parts.shape[1] - 2 * LANES, 1)


def rows_of(*blocks):
    return jnp.concatenate([array[head] for array, head in blocks], axis=0)


def store(out, parts, log_weights, lane):
    for h, part in enumerate(parts):
        out[h] = part.astype(out.dtype)
    out[len(parts)] = split_table(table_of(log_weights, lane), lane)


def store_local(out, table, parts, log_weights, lane):
    for h, part in enumerate(parts):
        out[h] = part
    table[...] = table_of(log_weights, lane)


def where_am_i():
    span = lax.axis_index("span")
    return span, 2 * span + lax.axis_index("head") // 2


def unless(seen):
    return jnp.where(seen, 0.0, -jnp.inf)


def first_kernel(queries, key_rows, x1, y1, held, sems):
    span, _ = where_am_i()
    half = x1.shape[0]

    def fetch(array, start, slot):
        source = array.at[:, pl.ds(start, half), :]
        return pltpu.make_async_copy(source, held.at[slot], sems.at[slot])

    def load(array, starts):
        for slot, start in enumerate(starts):
            fetch(array, start, slot).start()

    @pl.when(span == 0)
    def _():
        load(key_rows, (0, half))

    @pl.when(span == 1)
    def _():
        load(queries, (0, 0))

    for slot, out in enumerate((x1, y1)):
        fetch(queries, 0, slot).wait()
        for h in range(0, half, TILE):
            out[h : h + TILE] = jnp.swapaxes(held[slot, :, h : h + TILE, :], 0, 1)


def second_kernel(lent, q, k, v, x2, y2, x3, x4):
    span, block = where_am_i()
    half = x2.shape[0]
    y2[...] = v[half:]
    x4[...] = v[half + lent :]

    @pl.when(span == 0)
    def _():
        x2[...] = v[:half]

    @pl.when(span == 1)
    def _():
        x2[...] = q[half:]

    @pl.when(block == 0)
    def _():
        x3[...] = k[half + lent :]

    @pl.when(block != 0)
    def _():
        x3[: half - lent] = q[half : 2 * half - lent]


def choose_kernel(x1, y1, x2, y2, keys, visitor, values):
    span, _ = where_am_i()

    @pl.when(span == 0)
    def _():
        keys[...] = x1[...]
        visitor[...] = y1[...]
        values[...] = x2[...]

    @pl.when(span == 1)
    def _():
        keys[...] = y1[...]
        visitor[...] = x2[...]
        values[...] = y2[...]


def own_kernel(factor, q, k0, k1, v0, v1, out, table):
    span, _ = where_am_i()
    rows, width = q.shape[1:]
    half = out.shape[0]
    heads = [(1 - span) * half + h for h in range(half)]
    jobs = [(q[h], rows_of((k0, h), (k1, h)), rows_of((v0, h), (v1, h))) for h in heads]
    store_local(out, table, *attend(jobs, factor), lanes_of(rows, width))


def two_blocks(q, received, own, span, half, seen_received, seen_own):
    rk0, rk1, rv0, rv1 = received
    k0, k1, v0, v1 = own
    keys = 4 * rk0.shape[1]
    place = lax.broadcasted_iota(jnp.int32, (1, keys), 1)
    shift = jnp.where(place < keys // 2, unless(seen_received), unless(seen_own))
    jobs = []
    for h in range(half):
        g = span * half + h
        jobs.append(
            (
                q(h, g),
                rows_of((rk0, h), (rk1, h), (k0, g), (k1, g)),
                rows_of((rv0, h), (rv1, h), (v0, g), (v1, g)),
            )
        )
    return jobs, shift


def visit_kernel(factor, q, rk0, rk1, rv0, rv1, k0, k1, v0, v1, out):
    span, block = where_am_i()
    half, rows, width = q.shape
    jobs, shift = two_blocks(
        lambda h, g: q[h], (rk0, rk1, rv0, rv1), (k0, k1, v0, v1), span, half, block >= 0, block != 3
    )
    store(out, *attend(jobs, factor, shift), lanes_of(rows, width))


def stay_kernel(factor, q, rk0, rk1, rv0, rv1, k0, k1, v0, v1, out, table):
    span, block = where_am_i()
    rows, width = q.shape[1:]
    jobs, shift = two_blocks(
        lambda h, g: q[g], (rk0, rk1, rv0, rv1), (k0, k1, v0, v1), span, out.shape[0], block != 0, block >= 0
    )
    store_local(out, table, *attend(jobs, factor, shift), lanes_of(rows, width))


def guest_kernel(factor, host, first, q, k0, k1, v0, v1, out):
    _, block = where_am_i()
    heads, rows, width = q.shape

    @pl.when(block == host)
    def _():
        jobs = [
            (q[h], rows_of((k0, first + h), (k1, first + h)), rows_of((v0, first + h), (v1, first + h)))
            for h in range(heads)
        ]
        store(out, *attend(jobs, factor), lanes_of(rows, width))


def fetched_kernel(factor, host, first, q, k0, k1, v0, v1, out, table):
    _, block = where_am_i()
    heads, rows, width = out.shape

    @pl.when(block == host)
    def _():
        jobs = [(q[first + h], rows_of((k0, h), (k1, h)), rows_of((v0, h), (v1, h))) for h in range(heads)]
        store_local(out, table, *attend(jobs, factor), lanes_of(rows, width))


def merge_kernel(
    levels, gate_table, other, other_table, mine, mine_table, upper, across, extra, lent, fetched, fetched_table, out
):
    span, block = where_am_i()
    half, _, width = mine.shape
    lent_heads = half - fetched.shape[0]
    level = levels[span]
    lane = lanes_of(1, width)

    def finish(first, sources, last=half, begin=0):
        gates = jnp.zeros((1, width), jnp.float32)
        for h in range(begin, last):
            gates = jnp.where(lane == h, gate_table[level, first + h], gates)
        logs = [table for _, table, _ in sources]
        top = functools.reduce(jnp.maximum, logs)
        scaled = [jnp.exp2(table - top) for table in logs]
        ratio = gates / sum(scaled)
        scaled = [s * ratio for s in scaled]
        for start in range(begin, last, TILE // 2):
            sums = [
                sum(
                    parts[h - skip].astype(jnp.float32) * s[:, h : h + 1]
                    for (parts, _, skip), s in zip(sources, scaled)
                )
                for h in range(start, start + TILE // 2)
            ]
            together = jnp.swapaxes(jnp.stack(sums), 0, 1)
            out[:, first + start : first + start + TILE // 2, :] = together.astype(out.dtype)

    def sent(slab, shift=0.0):
        return slab, joined(slab[slab.shape[0] - 1]) + shift, 0

    def kept(parts, table):
        return parts, table[...], 0

    @pl.when(span == 1)
    def _():
        finish(0, [kept(other, other_table), sent(upper), sent(extra, unless(block == 3))])
        finish(half, [kept(mine, mine_table), sent(across)])

    @pl.when(block == 0)
    def _():
        finish(0, [kept(mine, mine_table)])
        finish(half, [kept(other, other_table)])

    @pl.when(block == 1)
    def _():
        finish(0, [kept(mine, mine_table)])
        finish(half, [kept(other, other_table), sent(lent)], last=lent_heads)
        moved = pltpu.roll(fetched_table[...], lent_heads, 1)
        finish(half, [kept(other, other_table), (fetched, moved, lent_heads)], begin=lent_heads)


def run(kernel, out_shape, operands, scalars=(), space=pltpu.VMEM, scratch=()):
    in_vmem, in_smem = pl.BlockSpec(memory_space=pltpu.VMEM), pl.BlockSpec(memory_space=pltpu.SMEM)
    return pl.pallas_call(
        kernel,
        out_shape=out_shape,
        in_specs=[in_smem] * len(scalars) + [pl.BlockSpec(memory_space=space)] * len(operands),
        out_specs=jax.tree.map(lambda _: in_vmem, out_shape),
        scratch_shapes=scratch,
        compiler_params=pltpu.CompilerParams(vmem_limit_bytes=8 << 20),
        cost_estimate=pl.CostEstimate(flops=2_000_000_000, bytes_accessed=1 << 20, transcendentals=0),
    )(*scalars, *operands)


def by_block(queries, key_rows, value_rows, noise_levels, gate_table):
    rows, heads, width = queries.shape
    half = heads // 2
    lent = half // 2
    per_span = lax.axis_size("head")
    share = per_span // 2
    factor = math.log2(math.e) / math.sqrt(width)
    devices = range(2 * per_span)

    def send(block, target):
        route = [(p, target(p)) for p in devices if target(p) is not None]
        return lax.ppermute(block, ("span", "head"), route)

    def sideways(p):
        return p ^ share

    def other_span(p):
        return p ^ per_span

    def partner(p):
        return p ^ 1

    def only(numbers, target):
        return lambda p: target(p) if p // share in numbers else None

    def up(p):
        return p + per_span if p < per_span else None

    def moved(block, target):
        return send(block, target)

    def by_head_first(a):
        return jnp.transpose(a, (1, 0, 2))

    def blocks(*counts):
        return tuple(jax.ShapeDtypeStruct((n, rows, width), jnp.bfloat16) for n in counts)

    def kernel(body, out_shape, *operands, **more):
        return run(body, out_shape, operands, **more)

    x1, y1 = kernel(
        first_kernel,
        blocks(half, half),
        queries,
        key_rows,
        space=pl.ANY,
        scratch=[pltpu.VMEM((2, rows, half, width), jnp.bfloat16), pltpu.SemaphoreType.DMA((2,))],
    )
    x1, y1, *raw = lax.optimization_barrier((x1, y1, queries, key_rows, value_rows))
    q, k, v = map(by_head_first, raw)
    x2, y2, x3, x4 = kernel(
        functools.partial(second_kernel, lent), blocks(half, half, half - lent, half - lent), q, k, v
    )
    x1 = moved(x1, only((0, 1, 3), sideways))
    y1 = moved(y1, other_span)
    own_k, own_v = moved(k, partner), moved(v, partner)
    x2 = moved(x2, sideways)
    y2 = moved(y2, other_span)
    x3 = moved(x3, only((0, 1), sideways))
    x4 = moved(x4, only((0,), sideways))

    def slab(n):
        return jax.ShapeDtypeStruct((n + 1, rows, width), jnp.bfloat16)

    def kept(n):
        return (
            jax.ShapeDtypeStruct((n, rows, width), jnp.float32),
            jax.ShapeDtypeStruct((rows, width), jnp.float32),
        )

    own = (k, own_k, v, own_v)
    other = kernel(functools.partial(own_kernel, factor), kept(half), q, *own)
    extra = kernel(functools.partial(guest_kernel, factor, 2, 0), slab(half), x1, *own)
    extra = moved(extra, only((2,), sideways))

    got_k, visitor, got_v = kernel(choose_kernel, blocks(half, half, half), x1, y1, x2, y2)
    got_k1, got_v1 = moved(got_k, partner), moved(got_v, partner)
    received = (got_k, got_k1, got_v, got_v1)
    away = kernel(functools.partial(visit_kernel, factor), slab(half), visitor, *received, *own)
    upper = moved(away, up)
    across = moved(away, only((2, 3), sideways))
    mine = kernel(functools.partial(stay_kernel, factor), kept(half), q, *received, *own)

    helped = kernel(functools.partial(guest_kernel, factor, 0, half), slab(lent), x3, *own)
    helped = moved(helped, only((0,), sideways))
    x3_1, x4_1 = (moved(a, only((1,), partner)) for a in (x3, x4))
    fetched = kernel(
        functools.partial(fetched_kernel, factor, 1, half + lent), kept(half - lent), q, x3, x3_1, x4, x4_1
    )
    return run(
        merge_kernel,
        jax.ShapeDtypeStruct((rows, heads, width), jnp.bfloat16),
        (*other, *mine, upper, across, extra, helped, *fetched),
        (noise_levels, gate_table),
    )


def body(queries, key_rows, value_rows, noise_levels, gate_table):
    rows, heads, _ = queries.shape
    spans, per_span = lax.axis_size("span"), lax.axis_size("head")
    two_by_two = spans == 2 and 2 * rows == BLOCK and per_span * rows == 2 * BLOCK
    if two_by_two and heads % (2 * TILE) == 0 and heads <= 2 * LANES:
        return by_block(queries, key_rows, value_rows, noise_levels, gate_table)
    return by_head(queries, key_rows, value_rows, noise_levels, gate_table)


def solution(mesh):
    tokens = ("video", "span", "head")
    return jax.shard_map(
        body,
        mesh=mesh,
        in_specs=(
            P(tokens, None, None),
            P(tokens, None, None),
            P(tokens, None, None),
            P("video"),
            P(),
        ),
        out_specs=P(tokens, None, None),
        check_vma=False,
    )
```

```python
import functools
import math

import jax
import jax.numpy as jnp
from jax import lax
from jax.experimental import pallas as pl
from jax.experimental.pallas import tpu as pltpu
from jax.sharding import PartitionSpec as P

BLOCK = 128
LEVELS = 8
ROOM = 62 << 20
TILE = 8
LANES = 32


def from_behind(block, axis, distance):
    devices = range(lax.axis_size(axis))
    route = [(i - distance, i) for i in devices if i - distance in devices]
    return lax.ppermute(block, axis, route)


def gate_rows_for(noise_levels, gate_table):
    one_hot = (jnp.arange(LEVELS, dtype=jnp.int32)[None, :] == noise_levels[:, None]).astype(
        jnp.float32
    )
    return jnp.dot(one_hot, gate_table, precision=lax.Precision.HIGHEST)


def by_head(queries, key_rows, value_rows, noise_levels, gate_table):
    row_count, head_count, head_width = queries.shape
    head_groups = lax.axis_size("head")
    per_group = head_count // head_groups
    chain_len = lax.axis_size("span")
    chain_pos = lax.axis_index("span")
    score_scale = 1.0 / math.sqrt(head_width)
    split_shape = (row_count, head_groups, per_group, head_width)
    query_heads, key_heads, value_heads = (
        lax.all_to_all(
            queries.reshape(split_shape), "head", split_axis=1, concat_axis=0, tiled=True
        ),
        lax.all_to_all(
            key_rows.reshape(split_shape), "head", split_axis=1, concat_axis=0, tiled=True
        ),
        lax.all_to_all(
            value_rows.reshape(split_shape), "head", split_axis=1, concat_axis=0, tiled=True
        ),
    )
    span_len = row_count * head_groups
    query_heads = query_heads.reshape(span_len, per_group, head_width)
    key_heads = key_heads.reshape(span_len, per_group, head_width)
    value_heads = value_heads.reshape(span_len, per_group, head_width)
    own_scores = (
        jnp.einsum("qhd,khd->qhk", query_heads, key_heads, preferred_element_type=jnp.float32)
        * score_scale
    )
    query_block = jnp.arange(span_len, dtype=jnp.int32) // BLOCK
    visible = (query_block[None, :] <= query_block[:, None])[:, None, :]
    own_max = jnp.max(jnp.where(visible, own_scores, -jnp.inf), axis=-1)
    own_weights = jnp.where(visible, jnp.exp(own_scores - own_max[..., None]), 0.0)
    own_totals = jnp.sum(own_weights, axis=-1)
    own_acc = jnp.einsum(
        "qhk,khd->qhd",
        own_weights.astype(jnp.bfloat16),
        value_heads,
        preferred_element_type=jnp.float32,
    )
    running = (own_max, own_totals, own_acc)

    def update(state_now, key_block, value_block):
        row_max, totals, accum = state_now
        scores = (
            jnp.einsum("qhd,khd->qhk", query_heads, key_block, preferred_element_type=jnp.float32)
            * score_scale
        )
        new_max = jnp.maximum(row_max, jnp.max(scores, axis=-1))
        rescale = jnp.exp(row_max - new_max)
        weights = jnp.exp(scores - new_max[..., None])
        totals = totals * rescale + jnp.sum(weights, axis=-1)
        accum = accum * rescale[..., None] + jnp.einsum(
            "qhk,khd->qhd",
            weights.astype(jnp.bfloat16),
            value_block,
            preferred_element_type=jnp.float32,
        )
        return (new_max, totals, accum)

    def advance(state_now, inputs):
        key_block, value_block, span_id = inputs
        useful = (span_id >= 0) & (span_id < chain_pos)
        return (
            lax.cond(
                useful,
                lambda inner: update(inner, key_block, value_block),
                lambda inner: inner,
                state_now,
            ),
            None,
        )

    def relay_turn(turn, loop_state):
        state_now, in_hand = loop_state
        in_hand = from_behind(in_hand, "span", 1)
        state_now, _ = advance(state_now, (in_hand[0], in_hand[1], chain_pos - 1 - turn))
        return (state_now, in_hand)

    running, _ = lax.fori_loop(
        0, chain_len - 1, relay_turn, (running, jnp.stack((key_heads, value_heads)))
    )
    _, totals, accum = running
    gate_rows = gate_rows_for(noise_levels, gate_table)
    gate_row = lax.dynamic_index_in_dim(gate_rows, chain_pos, 0, keepdims=False)
    my_gates = lax.dynamic_slice_in_dim(gate_row, lax.axis_index("head") * per_group, per_group, 0)
    result = (accum / totals[..., None] * my_gates[None, :, None]).astype(jnp.bfloat16)
    returned = lax.all_to_all(
        result.reshape(span_len, 1, per_group, head_width),
        "head",
        split_axis=0,
        concat_axis=1,
        tiled=True,
    )
    return returned.reshape(row_count, head_count, head_width)


def attend(jobs, factor, shift=None):
    scores = [
        lax.dot_general(q, k, (((1,), (1,)), ((), ())), preferred_element_type=jnp.float32)
        for q, k, _ in jobs
    ]
    if shift is not None:
        scores = [s + shift for s in scores]
    tops = [jnp.max(s, axis=1, keepdims=True) for s in scores]
    weights = [jnp.exp2((s - top) * factor) for s, top in zip(scores, tops)]
    totals = [jnp.sum(w, axis=1, keepdims=True) for w in weights]
    sums = [
        lax.dot_general(
            w.astype(jnp.bfloat16), v, (((1,), (0,)), ((), ())), preferred_element_type=jnp.float32
        )
        for w, (_, _, v) in zip(weights, jobs)
    ]
    return (
        [s * (1.0 / t) for s, t in zip(sums, totals)],
        [top * factor + jnp.log2(t) for top, t in zip(tops, totals)],
    )


def lanes_of(rows, width):
    return lax.broadcasted_iota(jnp.int32, (rows, width), 1)


def table_of(columns, lane):
    table = jnp.zeros(lane.shape, jnp.float32)
    for h, column in enumerate(columns):
        table = jnp.where(lane % LANES == h, column, table)
    return table


def split_table(table, lane):
    high = table.astype(jnp.bfloat16).astype(jnp.float32)
    rest = table - high
    middle = rest.astype(jnp.bfloat16).astype(jnp.float32)
    parts = jnp.where(lane < LANES, high, jnp.where(lane < 2 * LANES, middle, rest - middle))
    return jnp.where(lane < 3 * LANES, parts, 0.0).astype(jnp.bfloat16)


def joined(table):
    parts = table.astype(jnp.float32)
    return parts + pltpu.roll(parts, parts.shape[1] - LANES, 1) + pltpu.roll(parts, parts.shape[1] - 2 * LANES, 1)


def rows_of(*blocks):
    return jnp.concatenate([array[head] for array, head in blocks], axis=0)


def store(out, parts, log_weights, lane):
    for h, part in enumerate(parts):
        out[h] = part.astype(out.dtype)
    out[len(parts)] = split_table(table_of(log_weights, lane), lane)


def store_local(out, table, parts, log_weights, lane):
    for h, part in enumerate(parts):
        out[h] = part
    table[...] = table_of(log_weights, lane)


def where_am_i():
    span = lax.axis_index("span")
    return span, 2 * span + lax.axis_index("head") // 2


def unless(seen):
    return jnp.where(seen, 0.0, -jnp.inf)


def first_kernel(queries, key_rows, value_rows, x1, y1, held, sems):
    span, _ = where_am_i()
    half = x1.shape[0]
    part = half // 2

    def fetch(array, start, count, slot, place=0):
        source = array.at[:, pl.ds(start, count), :]
        return pltpu.make_async_copy(source, held.at[slot, :, pl.ds(place, count), :], sems.at[slot])

    @pl.when(span == 0)
    def _():
        for slot in range(2):
            fetch(key_rows, slot * half, TILE * 2, slot).start()
            fetch(value_rows, slot * half, TILE * 2, slot, TILE * 2).start()

    @pl.when(span == 1)
    def _():
        fetch(queries, 0, TILE * 4, 0).start()
        fetch(queries, 0, TILE * 4, 1).start()

    for slot, out in enumerate((x1, y1)):
        fetch(queries, 0, TILE * 4, slot).wait()

        def turned(start):
            return jnp.swapaxes(held[slot, :, start : start + TILE, :], 0, 1)

        @pl.when(span == 0)
        def _():
            for base, place in ((0, 0), (2 * TILE, part)):
                out[place : place + TILE] = turned(base)
                out[place + TILE : place + part] = turned(base + TILE)[: part - TILE]

        @pl.when(span == 1)
        def _():
            for start in range(0, half, TILE):
                out[start : start + TILE] = turned(start)


def second_kernel(q, k, v, x2, x3, y2, x4):
    span, block = where_am_i()
    part = x2.shape[0]
    half = 2 * part
    lent = x4.shape[0]
    y2[:part] = k[half + part :]
    y2[part:] = v[half + part :]

    @pl.when(span == 0)
    def _():
        x2[...] = k[part:half]
        x3[...] = v[part:half]

    @pl.when(span == 1)
    def _():
        x2[...] = q[half : half + part]
        x3[...] = q[half + part :]

    @pl.when(block == 0)
    def _():
        x4[: lent // 2] = k[half + lent :]
        x4[lent // 2 :] = v[half + lent :]

    @pl.when(block != 0)
    def _():
        x4[...] = q[half : half + lent]


def choose_kernel(x, y, out):
    span, _ = where_am_i()

    @pl.when(span == 0)
    def _():
        out[...] = x[...]

    @pl.when(span == 1)
    def _():
        out[...] = y[...]


def choose_second_kernel(x2, x3, y2, out):
    span, _ = where_am_i()
    part = x2.shape[0]

    @pl.when(span == 0)
    def _():
        out[:part] = x2[...]
        out[part:] = x3[...]

    @pl.when(span == 1)
    def _():
        out[...] = y2[...]


def own_kernel(factor, levels, gate_table, q, k0, k1, v0, v1, out, table, gates):
    span, _ = where_am_i()
    rows, width = q.shape[1:]
    half = out.shape[0]
    heads = [(1 - span) * half + h for h in range(half)]
    jobs = [(q[h], rows_of((k0, h), (k1, h)), rows_of((v0, h), (v1, h))) for h in heads]
    store_local(out, table, *attend(jobs, factor), lanes_of(rows, width))
    level = levels[span]
    lane = lanes_of(1, width)
    for group in range(2):
        row = jnp.zeros((1, width), jnp.float32)
        for h in range(half):
            row = jnp.where(lane == h, gate_table[level, group * half + h], row)
        gates[group : group + 1] = row


def hide(keys, seen_first, seen_second):
    place = lax.broadcasted_iota(jnp.int32, (1, keys), 1)
    return jnp.where(place < keys // 2, unless(seen_first), unless(seen_second))


def visit_kernel(factor, chunk, y1, x, got, got1, k0, k1, v0, v1, out, q):
    span, block = where_am_i()
    part, rows, width = x.shape

    @pl.when(span == 0)
    def _():
        q[...] = y1[chunk * part : (chunk + 1) * part]

    @pl.when(span == 1)
    def _():
        q[...] = x[...]

    jobs = []
    for h in range(part):
        g = (2 * span + chunk) * part + h
        jobs.append(
            (
                q[h],
                rows_of((got, h), (got1, h), (k0, g), (k1, g)),
                rows_of((got, part + h), (got1, part + h), (v0, g), (v1, g)),
            )
        )
    shift = hide(4 * rows, block >= 0, block != 3)
    store(out, *attend(jobs, factor, shift), lanes_of(rows, width))


def stay_kernel(factor, q, a, a1, b, b1, k0, k1, v0, v1, out, table):
    span, block = where_am_i()
    rows, width = q.shape[1:]
    half = out.shape[0]
    part = half // 2
    jobs = []
    for h in range(half):
        g = span * half + h
        first, second = (a, a1) if h < part else (b, b1)
        i = h % part
        jobs.append(
            (
                q[g],
                rows_of((first, i), (second, i), (k0, g), (k1, g)),
                rows_of((first, part + i), (second, part + i), (v0, g), (v1, g)),
            )
        )
    shift = hide(4 * rows, block != 0, block >= 0)
    store_local(out, table, *attend(jobs, factor, shift), lanes_of(rows, width))


def guest_kernel(factor, host, first, q, k0, k1, v0, v1, out):
    _, block = where_am_i()
    heads, rows, width = q.shape

    @pl.when(block == host)
    def _():
        jobs = [
            (q[h], rows_of((k0, first + h), (k1, first + h)), rows_of((v0, first + h), (v1, first + h)))
            for h in range(heads)
        ]
        store(out, *attend(jobs, factor), lanes_of(rows, width))


def fetched_kernel(factor, host, first, q, got, got1, out, table):
    _, block = where_am_i()
    heads, rows, width = out.shape

    @pl.when(block == host)
    def _():
        jobs = [
            (q[first + h], rows_of((got, h), (got1, h)), rows_of((got, heads + h), (got1, heads + h)))
            for h in range(heads)
        ]
        store_local(out, table, *attend(jobs, factor), lanes_of(rows, width))


def merged(gate_row, logs, parts_of, half, held, group, out, sem):
    top = functools.reduce(jnp.maximum, logs)
    scaled = [jnp.exp2(table - top) for table in logs]
    ratio = gate_row / sum(scaled)
    scaled = [s * ratio for s in scaled]
    for start in range(0, half, TILE):
        sums = [
            sum(part.astype(jnp.float32) * s[:, h : h + 1] for part, s in zip(parts_of(h), scaled))
            for h in range(start, start + TILE)
        ]
        together = jnp.swapaxes(jnp.stack(sums), 0, 1)
        held[:, start : start + TILE, :] = together.astype(held.dtype)
    leave(held, out, group, sem).start()


def leave(held, out, group, sem):
    half = held.shape[1]
    return pltpu.make_async_copy(held, out.at[:, pl.ds(group * half, half), :], sem)


def logs_of(slab):
    return joined(slab[slab.shape[0] - 1])


def side_by_side(first, second, count):
    lane = lanes_of(*first.shape)
    return jnp.where(lane < count, first, pltpu.roll(second, count, 1))


def picked(first, second, h, count):
    return first[h] if h < count else second[h - count]


def merge_first_kernel(gates, other, other_table, mine, mine_table, upper, upper2, extra, out, held, sem):
    span, block = where_am_i()
    half = mine.shape[0]
    part = half // 2
    gate_row = gates[0:1]

    @pl.when(span == 1)
    def _():
        logs = [
            other_table[...],
            side_by_side(logs_of(upper), logs_of(upper2), part),
            logs_of(extra) + unless(block == 3),
        ]
        merged(
            gate_row,
            logs,
            lambda h: [other[h], picked(upper, upper2, h, part), extra[h]],
            half, held, 0, out, sem,
        )

    @pl.when(span == 0)
    def _():
        merged(gate_row, [mine_table[...]], lambda h: [mine[h]], half, held, 0, out, sem)

    leave(held, out, 0, sem).wait()


def merge_second_kernel(
    gates, other, other_table, mine, mine_table, across, across2, lent, fetched, fetched_table, _, out, held, sem
):
    span, block = where_am_i()
    half = mine.shape[0]
    part = half // 2
    lent_heads = half - fetched.shape[0]
    gate_row = gates[1:2]

    @pl.when(span == 1)
    def _():
        logs = [mine_table[...], side_by_side(logs_of(across), logs_of(across2), part)]
        merged(
            gate_row, logs, lambda h: [mine[h], picked(across, across2, h, part)], half, held, 1, out, sem
        )

    @pl.when(block == 0)
    def _():
        merged(gate_row, [other_table[...]], lambda h: [other[h]], half, held, 1, out, sem)

    @pl.when(block == 1)
    def _():
        logs = [other_table[...], side_by_side(logs_of(lent), fetched_table[...], lent_heads)]
        merged(
            gate_row, logs, lambda h: [other[h], picked(lent, fetched, h, lent_heads)], half, held, 1, out, sem
        )

    leave(held, out, 1, sem).wait()


def run(
    kernel, out_shape, operands, scalars=(), space=pltpu.VMEM, scratch=(), room=8 << 20, out_space=pltpu.VMEM, into=None
):
    in_smem, anywhere = pl.BlockSpec(memory_space=pltpu.SMEM), pl.BlockSpec(memory_space=pl.ANY)
    inputs = [in_smem] * len(scalars) + [pl.BlockSpec(memory_space=space)] * len(operands)
    operands = [*scalars, *operands]
    if into is not None:
        operands.append(into)
        inputs.append(anywhere)
    return pl.pallas_call(
        kernel,
        out_shape=out_shape,
        in_specs=inputs,
        out_specs=jax.tree.map(lambda _: pl.BlockSpec(memory_space=out_space), out_shape),
        scratch_shapes=scratch,
        input_output_aliases={} if into is None else {len(operands) - 1: 0},
        compiler_params=pltpu.CompilerParams(vmem_limit_bytes=room),
        cost_estimate=pl.CostEstimate(flops=2_000_000_000, bytes_accessed=1 << 20, transcendentals=0),
    )(*operands)


def by_block(queries, key_rows, value_rows, noise_levels, gate_table):
    rows, heads, width = queries.shape
    half = heads // 2
    part = half // 2
    lent = 2 * (half // 3)
    per_span = lax.axis_size("head")
    share = per_span // 2
    factor = math.log2(math.e) / math.sqrt(width)
    devices = range(2 * per_span)

    def moved(block, target):
        route = [(p, target(p)) for p in devices if target(p) is not None]
        return lax.ppermute(block, ("span", "head"), route)

    def sideways(p):
        return p ^ share

    def other_span(p):
        return p ^ per_span

    def partner(p):
        return p ^ 1

    def only(numbers, target):
        return lambda p: target(p) if p // share in numbers else None

    def blocks(*counts):
        return tuple(jax.ShapeDtypeStruct((n, rows, width), jnp.bfloat16) for n in counts)

    def slab(n):
        return blocks(n + 1)[0]

    def kept(n):
        return (
            jax.ShapeDtypeStruct((n, rows, width), jnp.float32),
            jax.ShapeDtypeStruct((rows, width), jnp.float32),
        )

    def kernel(body, out_shape, *operands, **more):
        return run(body, out_shape, operands, **more)

    x1, y1 = kernel(
        first_kernel,
        blocks(half, half),
        queries,
        key_rows,
        value_rows,
        space=pl.ANY,
        room=ROOM,
        scratch=[pltpu.VMEM((2, rows, 4 * TILE, width), jnp.bfloat16), pltpu.SemaphoreType.DMA((2,))],
    )
    x1, y1, *raw = lax.optimization_barrier((x1, y1, queries, key_rows, value_rows))
    q, k, v = (jnp.transpose(a, (1, 0, 2)) for a in raw)
    x2, x3, y2, x4 = kernel(second_kernel, blocks(part, part, half, lent), q, k, v)
    x1 = moved(x1, only((0, 1, 3), sideways))
    y1 = moved(y1, other_span)
    own_k, own_v = moved(k, partner), moved(v, partner)
    x2, x3 = moved(x2, sideways), moved(x3, sideways)
    y2 = moved(y2, other_span)
    x4 = moved(x4, only((0, 1), sideways))

    own = (k, own_k, v, own_v)
    *other, gates = kernel(
        functools.partial(own_kernel, factor),
        (*kept(half), jax.ShapeDtypeStruct((2, width), jnp.float32)),
        q,
        *own,
        scalars=(noise_levels, gate_table),
    )
    a = kernel(choose_kernel, blocks(half)[0], x1, y1)
    a1 = moved(a, partner)
    extra = kernel(functools.partial(guest_kernel, factor, 2, 0), slab(half), x1, *own)
    extra = moved(extra, only((2,), sideways))

    def visit(chunk, x, got, got1):
        return kernel(
            functools.partial(visit_kernel, factor, chunk),
            slab(part),
            y1,
            x,
            got,
            got1,
            *own,
            scratch=[pltpu.VMEM((part, rows, width), jnp.bfloat16)],
        )

    away = visit(0, x2, a, a1)
    upper, across = moved(away, other_span), moved(away, only((2, 3), sideways))
    b = kernel(choose_second_kernel, blocks(half)[0], x2, x3, y2)
    b1 = moved(b, partner)
    away = visit(1, x3, b, b1)
    upper2, across2 = moved(away, other_span), moved(away, only((2, 3), sideways))
    helped = kernel(functools.partial(guest_kernel, factor, 0, half), slab(lent), x4, *own)
    helped = moved(helped, only((0,), sideways))
    x4_1 = moved(x4, only((1,), partner))
    mine = kernel(functools.partial(stay_kernel, factor), kept(half), q, a, a1, b, b1, *own)
    fetched = kernel(functools.partial(fetched_kernel, factor, 1, half + lent), kept(half - lent), q, x4, x4_1)
    outcome = jax.ShapeDtypeStruct((rows, heads, width), jnp.bfloat16)
    more = dict(
        out_space=pl.ANY,
        scratch=[pltpu.VMEM((rows, half, width), jnp.bfloat16), pltpu.SemaphoreType.DMA(())],
    )
    out = kernel(merge_first_kernel, outcome, gates, *other, *mine, upper, upper2, extra, **more)
    return kernel(
        merge_second_kernel, outcome, gates, *other, *mine, across, across2, helped, *fetched, into=out, **more
    )


def body(queries, key_rows, value_rows, noise_levels, gate_table):
    rows, heads, _ = queries.shape
    spans, per_span = lax.axis_size("span"), lax.axis_size("head")
    two_by_two = spans == 2 and 2 * rows == BLOCK and per_span * rows == 2 * BLOCK
    if two_by_two and heads == 6 * TILE:
        return by_block(queries, key_rows, value_rows, noise_levels, gate_table)
    return by_head(queries, key_rows, value_rows, noise_levels, gate_table)


def solution(mesh):
    tokens = ("video", "span", "head")
    return jax.shard_map(
        body,
        mesh=mesh,
        in_specs=(
            P(tokens, None, None),
            P(tokens, None, None),
            P(tokens, None, None),
            P("video"),
            P(),
        ),
        out_specs=P(tokens, None, None),
        check_vma=False,
    )
```

```python
import functools
import math

import jax
import jax.numpy as jnp
from jax import lax
from jax.experimental import pallas as pl
from jax.experimental.pallas import tpu as pltpu
from jax.sharding import PartitionSpec as P

BLOCK = 128
LEVELS = 8
ROOM = 62 << 20
TILE = 8
LANES = 32


def from_behind(block, axis, distance):
    devices = range(lax.axis_size(axis))
    route = [(i - distance, i) for i in devices if i - distance in devices]
    return lax.ppermute(block, axis, route)


def gate_rows_for(noise_levels, gate_table):
    one_hot = (jnp.arange(LEVELS, dtype=jnp.int32)[None, :] == noise_levels[:, None]).astype(
        jnp.float32
    )
    return jnp.dot(one_hot, gate_table, precision=lax.Precision.HIGHEST)


def by_head(queries, key_rows, value_rows, noise_levels, gate_table):
    row_count, head_count, head_width = queries.shape
    head_groups = lax.axis_size("head")
    per_group = head_count // head_groups
    chain_len = lax.axis_size("span")
    chain_pos = lax.axis_index("span")
    score_scale = 1.0 / math.sqrt(head_width)
    split_shape = (row_count, head_groups, per_group, head_width)
    query_heads, key_heads, value_heads = (
        lax.all_to_all(
            queries.reshape(split_shape), "head", split_axis=1, concat_axis=0, tiled=True
        ),
        lax.all_to_all(
            key_rows.reshape(split_shape), "head", split_axis=1, concat_axis=0, tiled=True
        ),
        lax.all_to_all(
            value_rows.reshape(split_shape), "head", split_axis=1, concat_axis=0, tiled=True
        ),
    )
    span_len = row_count * head_groups
    query_heads = query_heads.reshape(span_len, per_group, head_width)
    key_heads = key_heads.reshape(span_len, per_group, head_width)
    value_heads = value_heads.reshape(span_len, per_group, head_width)
    own_scores = (
        jnp.einsum("qhd,khd->qhk", query_heads, key_heads, preferred_element_type=jnp.float32)
        * score_scale
    )
    query_block = jnp.arange(span_len, dtype=jnp.int32) // BLOCK
    visible = (query_block[None, :] <= query_block[:, None])[:, None, :]
    own_max = jnp.max(jnp.where(visible, own_scores, -jnp.inf), axis=-1)
    own_weights = jnp.where(visible, jnp.exp(own_scores - own_max[..., None]), 0.0)
    own_totals = jnp.sum(own_weights, axis=-1)
    own_acc = jnp.einsum(
        "qhk,khd->qhd",
        own_weights.astype(jnp.bfloat16),
        value_heads,
        preferred_element_type=jnp.float32,
    )
    running = (own_max, own_totals, own_acc)

    def update(state_now, key_block, value_block):
        row_max, totals, accum = state_now
        scores = (
            jnp.einsum("qhd,khd->qhk", query_heads, key_block, preferred_element_type=jnp.float32)
            * score_scale
        )
        new_max = jnp.maximum(row_max, jnp.max(scores, axis=-1))
        rescale = jnp.exp(row_max - new_max)
        weights = jnp.exp(scores - new_max[..., None])
        totals = totals * rescale + jnp.sum(weights, axis=-1)
        accum = accum * rescale[..., None] + jnp.einsum(
            "qhk,khd->qhd",
            weights.astype(jnp.bfloat16),
            value_block,
            preferred_element_type=jnp.float32,
        )
        return (new_max, totals, accum)

    def advance(state_now, inputs):
        key_block, value_block, span_id = inputs
        useful = (span_id >= 0) & (span_id < chain_pos)
        return (
            lax.cond(
                useful,
                lambda inner: update(inner, key_block, value_block),
                lambda inner: inner,
                state_now,
            ),
            None,
        )

    def relay_turn(turn, loop_state):
        state_now, in_hand = loop_state
        in_hand = from_behind(in_hand, "span", 1)
        state_now, _ = advance(state_now, (in_hand[0], in_hand[1], chain_pos - 1 - turn))
        return (state_now, in_hand)

    running, _ = lax.fori_loop(
        0, chain_len - 1, relay_turn, (running, jnp.stack((key_heads, value_heads)))
    )
    _, totals, accum = running
    gate_rows = gate_rows_for(noise_levels, gate_table)
    gate_row = lax.dynamic_index_in_dim(gate_rows, chain_pos, 0, keepdims=False)
    my_gates = lax.dynamic_slice_in_dim(gate_row, lax.axis_index("head") * per_group, per_group, 0)
    result = (accum / totals[..., None] * my_gates[None, :, None]).astype(jnp.bfloat16)
    returned = lax.all_to_all(
        result.reshape(span_len, 1, per_group, head_width),
        "head",
        split_axis=0,
        concat_axis=1,
        tiled=True,
    )
    return returned.reshape(row_count, head_count, head_width)


def attend(jobs, factor, shift=None):
    scores = [
        lax.dot_general(q, k, (((1,), (1,)), ((), ())), preferred_element_type=jnp.float32)
        for q, k, _ in jobs
    ]
    if shift is not None:
        scores = [s + shift for s in scores]
    tops = [jnp.max(s, axis=1, keepdims=True) for s in scores]
    weights = [jnp.exp2((s - top) * factor) for s, top in zip(scores, tops)]
    totals = [jnp.sum(w, axis=1, keepdims=True) for w in weights]
    sums = [
        lax.dot_general(
            w.astype(jnp.bfloat16), v, (((1,), (0,)), ((), ())), preferred_element_type=jnp.float32
        )
        for w, (_, _, v) in zip(weights, jobs)
    ]
    return (
        [s * (1.0 / t) for s, t in zip(sums, totals)],
        [top * factor + jnp.log2(t) for top, t in zip(tops, totals)],
    )


def lanes_of(rows, width):
    return lax.broadcasted_iota(jnp.int32, (rows, width), 1)


def table_of(columns, lane):
    table = jnp.zeros(lane.shape, jnp.float32)
    for h, column in enumerate(columns):
        table = jnp.where(lane % LANES == h, column, table)
    return table


def split_table(table, lane):
    high = table.astype(jnp.bfloat16).astype(jnp.float32)
    rest = table - high
    middle = rest.astype(jnp.bfloat16).astype(jnp.float32)
    parts = jnp.where(lane < LANES, high, jnp.where(lane < 2 * LANES, middle, rest - middle))
    return jnp.where(lane < 3 * LANES, parts, 0.0).astype(jnp.bfloat16)


def joined(table):
    parts = table.astype(jnp.float32)
    return parts + pltpu.roll(parts, parts.shape[1] - LANES, 1) + pltpu.roll(parts, parts.shape[1] - 2 * LANES, 1)


def rows_of(*blocks):
    return jnp.concatenate([array[head] for array, head in blocks], axis=0)


def store(out, parts, log_weights, lane):
    for h, part in enumerate(parts):
        out[h] = part.astype(out.dtype)
    out[len(parts)] = split_table(table_of(log_weights, lane), lane)


def store_local(out, table, parts, log_weights, lane):
    for h, part in enumerate(parts):
        out[h] = part
    table[...] = table_of(log_weights, lane)


def where_am_i():
    span = lax.axis_index("span")
    return span, 2 * span + lax.axis_index("head") // 2


def unless(seen):
    return jnp.where(seen, 0.0, -jnp.inf)


def first_kernel(queries, key_rows, value_rows, x1, y1, held, sems):
    span, block = where_am_i()
    half = x1.shape[0]
    part = half // 2

    def fetch(array, start, count, slot, place=0):
        source = array.at[:, pl.ds(start, count), :]
        return pltpu.make_async_copy(source, held.at[slot, :, pl.ds(place, count), :], sems.at[slot])

    pairs = (block != 3, span == 0)
    for slot, of_keys in enumerate(pairs):

        @pl.when(of_keys)
        def _():
            fetch(key_rows, slot * half, TILE * 2, slot).start()
            fetch(value_rows, slot * half, TILE * 2, slot, TILE * 2).start()

        @pl.when(jnp.logical_not(of_keys))
        def _():
            fetch(queries, 0, TILE * 4, slot).start()

    for slot, (out, of_keys) in enumerate(zip((x1, y1), pairs)):
        fetch(queries, 0, TILE * 4, slot).wait()

        def turned(start):
            return jnp.swapaxes(held[slot, :, start : start + TILE, :], 0, 1)

        @pl.when(of_keys)
        def _():
            for base, place in ((0, 0), (2 * TILE, part)):
                out[place : place + TILE] = turned(base)
                out[place + TILE : place + part] = turned(base + TILE)[: part - TILE]

        @pl.when(jnp.logical_not(of_keys))
        def _():
            for start in range(0, half, TILE):
                out[start : start + TILE] = turned(start)


def second_kernel(q, k, v, x2, x3, y2, x4):
    span, block = where_am_i()
    part = x2.shape[0]
    half = 2 * part
    taken = x4.shape[0] // 2
    y2[:part] = k[half + part :]
    y2[part:] = v[half + part :]

    @pl.when(span == 0)
    def _():
        x2[...] = k[part:half]
        x3[...] = v[part:half]

    @pl.when(span == 1)
    def _():
        x2[...] = q[half : half + part]
        x3[...] = q[half + part :]

    @pl.when(block == 0)
    def _():
        x4[:taken] = k[2 * half - taken :]
        x4[taken:] = v[2 * half - taken :]

    @pl.when(block != 0)
    def _():
        x4[...] = q[half : half + 2 * taken]


def choose_kernel(x, y, out):
    span, _ = where_am_i()

    @pl.when(span == 0)
    def _():
        out[...] = x[...]

    @pl.when(span == 1)
    def _():
        out[...] = y[...]


def choose_second_kernel(x2, x3, y2, out):
    span, _ = where_am_i()
    part = x2.shape[0]

    @pl.when(span == 0)
    def _():
        out[:part] = x2[...]
        out[part:] = x3[...]

    @pl.when(span == 1)
    def _():
        out[...] = y2[...]


def own_kernel(factor, levels, gate_table, q, k0, k1, v0, v1, out, table, gates):
    span, _ = where_am_i()
    rows, width = q.shape[1:]
    half = out.shape[0]
    heads = [(1 - span) * half + h for h in range(half)]
    jobs = [(q[h], rows_of((k0, h), (k1, h)), rows_of((v0, h), (v1, h))) for h in heads]
    store_local(out, table, *attend(jobs, factor), lanes_of(rows, width))
    level = levels[span]
    lane = lanes_of(1, width)
    for group in range(2):
        row = jnp.zeros((1, width), jnp.float32)
        for h in range(half):
            row = jnp.where(lane == h, gate_table[level, group * half + h], row)
        gates[group : group + 1] = row


def hide(keys, seen_first, seen_second):
    place = lax.broadcasted_iota(jnp.int32, (1, keys), 1)
    return jnp.where(place < keys // 2, unless(seen_first), unless(seen_second))


def visit_kernel(factor, chunk, y1, x, got, got1, k0, k1, v0, v1, out, q):
    span, block = where_am_i()
    part, rows, width = x.shape

    @pl.when(span == 0)
    def _():
        q[...] = y1[chunk * part : (chunk + 1) * part]

    @pl.when(span == 1)
    def _():
        q[...] = x[...]

    jobs = []
    for h in range(part):
        g = (2 * span + chunk) * part + h
        jobs.append(
            (
                q[h],
                rows_of((got, h), (got1, h), (k0, g), (k1, g)),
                rows_of((got, part + h), (got1, part + h), (v0, g), (v1, g)),
            )
        )
    shift = hide(4 * rows, block >= 0, block != 3)
    store(out, *attend(jobs, factor, shift), lanes_of(rows, width))


def stay_kernel(factor, q, a, a1, b, b1, k0, k1, v0, v1, out, table):
    span, block = where_am_i()
    rows, width = q.shape[1:]
    half = out.shape[0]
    part = half // 2
    jobs = []
    for h in range(half):
        g = span * half + h
        first, second = (a, a1) if h < part else (b, b1)
        i = h % part
        jobs.append(
            (
                q[g],
                rows_of((first, i), (second, i), (k0, g), (k1, g)),
                rows_of((first, part + i), (second, part + i), (v0, g), (v1, g)),
            )
        )
    shift = hide(4 * rows, block != 0, block >= 0)
    store_local(out, table, *attend(jobs, factor, shift), lanes_of(rows, width))


def guest_kernel(factor, host, first, skip, q, k0, k1, v0, v1, out):
    _, block = where_am_i()
    heads, rows, width = out.shape[0] - 1, *q.shape[1:]

    @pl.when(block == host)
    def _():
        jobs = [
            (q[skip + h], rows_of((k0, first + h), (k1, first + h)), rows_of((v0, first + h), (v1, first + h)))
            for h in range(heads)
        ]
        store(out, *attend(jobs, factor), lanes_of(rows, width))


def fetched_kernel(factor, host, first, q, got, got1, out, table):
    _, block = where_am_i()
    heads, rows, width = out.shape

    @pl.when(block == host)
    def _():
        jobs = [
            (q[first + h], rows_of((got, h), (got1, h)), rows_of((got, heads + h), (got1, heads + h)))
            for h in range(heads)
        ]
        store_local(out, table, *attend(jobs, factor), lanes_of(rows, width))


def merged(gate_row, logs, parts_of, half, held, group, out, sem):
    top = functools.reduce(jnp.maximum, logs)
    scaled = [jnp.exp2(table - top) for table in logs]
    ratio = gate_row / sum(scaled)
    scaled = [s * ratio for s in scaled]
    for start in range(0, half, TILE):
        sums = [
            sum(part.astype(jnp.float32) * s[:, h : h + 1] for part, s in zip(parts_of(h), scaled))
            for h in range(start, start + TILE)
        ]
        together = jnp.swapaxes(jnp.stack(sums), 0, 1)
        held[:, start : start + TILE, :] = together.astype(held.dtype)
    leave(held, out, group, sem).start()


def leave(held, out, group, sem):
    half = held.shape[1]
    return pltpu.make_async_copy(held, out.at[:, pl.ds(group * half, half), :], sem)


def logs_of(slab):
    return joined(slab[slab.shape[0] - 1])


def side_by_side(first, second, count):
    lane = lanes_of(*first.shape)
    return jnp.where(lane < count, first, pltpu.roll(second, count, 1))


def picked(first, second, h, count):
    return first[h] if h < count else second[h - count]


def merge_first_kernel(
    gates, other, other_table, mine, mine_table, upper, upper2, extra, third, third_table, out, held, sem
):
    span, block = where_am_i()
    half = mine.shape[0]
    part = half // 2
    gate_row = gates[0:1]

    @pl.when(block == 2)
    def _():
        logs = [other_table[...], side_by_side(logs_of(upper), logs_of(upper2), part)]
        merged(
            gate_row, logs, lambda h: [other[h], picked(upper, upper2, h, part)], half, held, 0, out, sem
        )

    @pl.when(block == 3)
    def _():
        logs = [
            other_table[...],
            side_by_side(logs_of(upper), logs_of(upper2), part),
            side_by_side(third_table[...], logs_of(extra), part),
        ]
        merged(
            gate_row,
            logs,
            lambda h: [other[h], picked(upper, upper2, h, part), picked(third, extra, h, part)],
            half, held, 0, out, sem,
        )

    @pl.when(span == 0)
    def _():
        merged(gate_row, [mine_table[...]], lambda h: [mine[h]], half, held, 0, out, sem)

    leave(held, out, 0, sem).wait()


def merge_second_kernel(
    gates, other, other_table, mine, mine_table, across, across2, lent, fetched, fetched_table, _, out, held, sem
):
    span, block = where_am_i()
    half = mine.shape[0]
    part = half // 2
    lent_heads = half - fetched.shape[0]
    gate_row = gates[1:2]

    @pl.when(span == 1)
    def _():
        logs = [mine_table[...], side_by_side(logs_of(across), logs_of(across2), part)]
        merged(
            gate_row, logs, lambda h: [mine[h], picked(across, across2, h, part)], half, held, 1, out, sem
        )

    @pl.when(block == 0)
    def _():
        merged(gate_row, [other_table[...]], lambda h: [other[h]], half, held, 1, out, sem)

    @pl.when(block == 1)
    def _():
        logs = [other_table[...], side_by_side(logs_of(lent), fetched_table[...], lent_heads)]
        merged(
            gate_row, logs, lambda h: [other[h], picked(lent, fetched, h, lent_heads)], half, held, 1, out, sem
        )

    leave(held, out, 1, sem).wait()


def run(
    kernel, out_shape, operands, scalars=(), space=pltpu.VMEM, scratch=(), room=8 << 20, out_space=pltpu.VMEM, into=None
):
    in_smem, anywhere = pl.BlockSpec(memory_space=pltpu.SMEM), pl.BlockSpec(memory_space=pl.ANY)
    inputs = [in_smem] * len(scalars) + [pl.BlockSpec(memory_space=space)] * len(operands)
    operands = [*scalars, *operands]
    if into is not None:
        operands.append(into)
        inputs.append(anywhere)
    return pl.pallas_call(
        kernel,
        out_shape=out_shape,
        in_specs=inputs,
        out_specs=jax.tree.map(lambda _: pl.BlockSpec(memory_space=out_space), out_shape),
        scratch_shapes=scratch,
        input_output_aliases={} if into is None else {len(operands) - 1: 0},
        compiler_params=pltpu.CompilerParams(vmem_limit_bytes=room),
        cost_estimate=pl.CostEstimate(flops=2_000_000_000, bytes_accessed=1 << 20, transcendentals=0),
    )(*operands)


def by_block(queries, key_rows, value_rows, noise_levels, gate_table):
    rows, heads, width = queries.shape
    half = heads // 2
    part = half // 2
    lent = half // 2
    per_span = lax.axis_size("head")
    share = per_span // 2
    factor = math.log2(math.e) / math.sqrt(width)
    devices = range(2 * per_span)

    def moved(block, target):
        route = [(p, target(p)) for p in devices if target(p) is not None]
        return lax.ppermute(block, ("span", "head"), route)

    def sideways(p):
        return p ^ share

    def other_span(p):
        return p ^ per_span

    def partner(p):
        return p ^ 1

    def only(numbers, target):
        return lambda p: target(p) if p // share in numbers else None

    def up(p):
        return p + per_span if p < per_span else None

    def blocks(*counts):
        return tuple(jax.ShapeDtypeStruct((n, rows, width), jnp.bfloat16) for n in counts)

    def slab(n):
        return blocks(n + 1)[0]

    def kept(n):
        return (
            jax.ShapeDtypeStruct((n, rows, width), jnp.float32),
            jax.ShapeDtypeStruct((rows, width), jnp.float32),
        )

    def kernel(body, out_shape, *operands, **more):
        return run(body, out_shape, operands, **more)

    x1, y1 = kernel(
        first_kernel,
        blocks(half, half),
        queries,
        key_rows,
        value_rows,
        space=pl.ANY,
        room=ROOM,
        scratch=[pltpu.VMEM((2, rows, 4 * TILE, width), jnp.bfloat16), pltpu.SemaphoreType.DMA((2,))],
    )
    x1, y1, *raw = lax.optimization_barrier((x1, y1, queries, key_rows, value_rows))
    q, k, v = (jnp.transpose(a, (1, 0, 2)) for a in raw)
    x2, x3, y2, x4 = kernel(second_kernel, blocks(part, part, half, 2 * (half - lent)), q, k, v)
    x1 = moved(x1, sideways)
    y1 = moved(y1, other_span)
    own_k, own_v = moved(k, partner), moved(v, partner)
    x2, x3 = moved(x2, sideways), moved(x3, sideways)
    y2 = moved(y2, other_span)
    x4 = moved(x4, only((0, 1), sideways))

    own = (k, own_k, v, own_v)
    *other, gates = kernel(
        functools.partial(own_kernel, factor),
        (*kept(half), jax.ShapeDtypeStruct((2, width), jnp.float32)),
        q,
        *own,
        scalars=(noise_levels, gate_table),
    )
    a = kernel(choose_kernel, blocks(half)[0], x1, y1)
    a1 = moved(a, partner)
    x1_1 = moved(x1, only((3,), partner))
    extra = kernel(functools.partial(guest_kernel, factor, 2, part, part), slab(half - part), x1, *own)
    extra = moved(extra, only((2,), sideways))
    third = kernel(functools.partial(fetched_kernel, factor, 3, 0), kept(part), q, x1, x1_1)

    def visit(chunk, x, got, got1):
        return kernel(
            functools.partial(visit_kernel, factor, chunk),
            slab(part),
            y1,
            x,
            got,
            got1,
            *own,
            scratch=[pltpu.VMEM((part, rows, width), jnp.bfloat16)],
        )

    away = visit(0, x2, a, a1)
    upper, across = moved(away, other_span), moved(away, only((2, 3), sideways))
    b = kernel(choose_second_kernel, blocks(half)[0], x2, x3, y2)
    b1 = moved(b, partner)
    away = visit(1, x3, b, b1)
    upper2, across2 = moved(away, up), moved(away, only((2, 3), sideways))
    helped = kernel(functools.partial(guest_kernel, factor, 0, half, 0), slab(lent), x4, *own)
    helped = moved(helped, only((0,), sideways))
    x4_1 = moved(x4, only((1,), partner))
    mine = kernel(functools.partial(stay_kernel, factor), kept(half), q, a, a1, b, b1, *own)
    fetched = kernel(functools.partial(fetched_kernel, factor, 1, half + lent), kept(half - lent), q, x4, x4_1)
    outcome = jax.ShapeDtypeStruct((rows, heads, width), jnp.bfloat16)
    more = dict(
        out_space=pl.ANY,
        scratch=[pltpu.VMEM((rows, half, width), jnp.bfloat16), pltpu.SemaphoreType.DMA(())],
    )
    out = kernel(merge_first_kernel, outcome, gates, *other, *mine, upper, upper2, extra, *third, **more)
    return kernel(
        merge_second_kernel, outcome, gates, *other, *mine, across, across2, helped, *fetched, into=out, **more
    )


def body(queries, key_rows, value_rows, noise_levels, gate_table):
    rows, heads, _ = queries.shape
    spans, per_span = lax.axis_size("span"), lax.axis_size("head")
    two_by_two = spans == 2 and 2 * rows == BLOCK and per_span * rows == 2 * BLOCK
    if two_by_two and heads == 6 * TILE:
        return by_block(queries, key_rows, value_rows, noise_levels, gate_table)
    return by_head(queries, key_rows, value_rows, noise_levels, gate_table)


def solution(mesh):
    tokens = ("video", "span", "head")
    return jax.shard_map(
        body,
        mesh=mesh,
        in_specs=(
            P(tokens, None, None),
            P(tokens, None, None),
            P(tokens, None, None),
            P("video"),
            P(),
        ),
        out_specs=P(tokens, None, None),
        check_vma=False,
    )
```

```python
import functools
import math

import jax
import jax.numpy as jnp
from jax import lax
from jax.experimental import pallas as pl
from jax.experimental.pallas import tpu as pltpu
from jax.sharding import PartitionSpec as P

BLOCK = 128
LEVELS = 8
ROOM = 211 << 18
TILE = 8
LANES = 32


def from_behind(block, axis, distance):
    devices = range(lax.axis_size(axis))
    route = [(i - distance, i) for i in devices if i - distance in devices]
    return lax.ppermute(block, axis, route)


def gate_rows_for(noise_levels, gate_table):
    one_hot = (jnp.arange(LEVELS, dtype=jnp.int32)[None, :] == noise_levels[:, None]).astype(
        jnp.float32
    )
    return jnp.dot(one_hot, gate_table, precision=lax.Precision.HIGHEST)


def by_head(queries, key_rows, value_rows, noise_levels, gate_table):
    row_count, head_count, head_width = queries.shape
    head_groups = lax.axis_size("head")
    per_group = head_count // head_groups
    chain_len = lax.axis_size("span")
    chain_pos = lax.axis_index("span")
    score_scale = 1.0 / math.sqrt(head_width)
    split_shape = (row_count, head_groups, per_group, head_width)
    query_heads, key_heads, value_heads = (
        lax.all_to_all(
            queries.reshape(split_shape), "head", split_axis=1, concat_axis=0, tiled=True
        ),
        lax.all_to_all(
            key_rows.reshape(split_shape), "head", split_axis=1, concat_axis=0, tiled=True
        ),
        lax.all_to_all(
            value_rows.reshape(split_shape), "head", split_axis=1, concat_axis=0, tiled=True
        ),
    )
    span_len = row_count * head_groups
    query_heads = query_heads.reshape(span_len, per_group, head_width)
    key_heads = key_heads.reshape(span_len, per_group, head_width)
    value_heads = value_heads.reshape(span_len, per_group, head_width)
    own_scores = (
        jnp.einsum("qhd,khd->qhk", query_heads, key_heads, preferred_element_type=jnp.float32)
        * score_scale
    )
    query_block = jnp.arange(span_len, dtype=jnp.int32) // BLOCK
    visible = (query_block[None, :] <= query_block[:, None])[:, None, :]
    own_max = jnp.max(jnp.where(visible, own_scores, -jnp.inf), axis=-1)
    own_weights = jnp.where(visible, jnp.exp(own_scores - own_max[..., None]), 0.0)
    own_totals = jnp.sum(own_weights, axis=-1)
    own_acc = jnp.einsum(
        "qhk,khd->qhd",
        own_weights.astype(jnp.bfloat16),
        value_heads,
        preferred_element_type=jnp.float32,
    )
    running = (own_max, own_totals, own_acc)

    def update(state_now, key_block, value_block):
        row_max, totals, accum = state_now
        scores = (
            jnp.einsum("qhd,khd->qhk", query_heads, key_block, preferred_element_type=jnp.float32)
            * score_scale
        )
        new_max = jnp.maximum(row_max, jnp.max(scores, axis=-1))
        rescale = jnp.exp(row_max - new_max)
        weights = jnp.exp(scores - new_max[..., None])
        totals = totals * rescale + jnp.sum(weights, axis=-1)
        accum = accum * rescale[..., None] + jnp.einsum(
            "qhk,khd->qhd",
            weights.astype(jnp.bfloat16),
            value_block,
            preferred_element_type=jnp.float32,
        )
        return (new_max, totals, accum)

    def advance(state_now, inputs):
        key_block, value_block, span_id = inputs
        useful = (span_id >= 0) & (span_id < chain_pos)
        return (
            lax.cond(
                useful,
                lambda inner: update(inner, key_block, value_block),
                lambda inner: inner,
                state_now,
            ),
            None,
        )

    def relay_turn(turn, loop_state):
        state_now, in_hand = loop_state
        in_hand = from_behind(in_hand, "span", 1)
        state_now, _ = advance(state_now, (in_hand[0], in_hand[1], chain_pos - 1 - turn))
        return (state_now, in_hand)

    running, _ = lax.fori_loop(
        0, chain_len - 1, relay_turn, (running, jnp.stack((key_heads, value_heads)))
    )
    _, totals, accum = running
    gate_rows = gate_rows_for(noise_levels, gate_table)
    gate_row = lax.dynamic_index_in_dim(gate_rows, chain_pos, 0, keepdims=False)
    my_gates = lax.dynamic_slice_in_dim(gate_row, lax.axis_index("head") * per_group, per_group, 0)
    result = (accum / totals[..., None] * my_gates[None, :, None]).astype(jnp.bfloat16)
    returned = lax.all_to_all(
        result.reshape(span_len, 1, per_group, head_width),
        "head",
        split_axis=0,
        concat_axis=1,
        tiled=True,
    )
    return returned.reshape(row_count, head_count, head_width)


def attend(jobs, factor, shift=None):
    scores = [
        lax.dot_general(q, k, (((1,), (1,)), ((), ())), preferred_element_type=jnp.float32)
        for q, k, _ in jobs
    ]
    if shift is not None:
        scores = [s + shift for s in scores]
    tops = [jnp.max(s, axis=1, keepdims=True) for s in scores]
    weights = [jnp.exp2((s - top) * factor) for s, top in zip(scores, tops)]
    totals = [jnp.sum(w, axis=1, keepdims=True) for w in weights]
    sums = [
        lax.dot_general(
            w.astype(jnp.bfloat16), v, (((1,), (0,)), ((), ())), preferred_element_type=jnp.float32
        )
        for w, (_, _, v) in zip(weights, jobs)
    ]
    return (
        [s * (1.0 / t) for s, t in zip(sums, totals)],
        [top * factor + jnp.log2(t) for top, t in zip(tops, totals)],
    )


def lanes_of(rows, width):
    return lax.broadcasted_iota(jnp.int32, (rows, width), 1)


def table_of(columns, lane):
    table = jnp.zeros(lane.shape, jnp.float32)
    for h, column in enumerate(columns):
        table = jnp.where(lane % LANES == h, column, table)
    return table


def split_table(table, lane):
    high = table.astype(jnp.bfloat16).astype(jnp.float32)
    rest = table - high
    middle = rest.astype(jnp.bfloat16).astype(jnp.float32)
    parts = jnp.where(lane < LANES, high, jnp.where(lane < 2 * LANES, middle, rest - middle))
    return jnp.where(lane < 3 * LANES, parts, 0.0).astype(jnp.bfloat16)


def joined(table):
    parts = table.astype(jnp.float32)
    return parts + pltpu.roll(parts, parts.shape[1] - LANES, 1) + pltpu.roll(parts, parts.shape[1] - 2 * LANES, 1)


def rows_of(*blocks):
    return jnp.concatenate([array[head] for array, head in blocks], axis=0)


def store(out, parts, log_weights, lane):
    for h, part in enumerate(parts):
        out[h] = part.astype(out.dtype)
    out[len(parts)] = split_table(table_of(log_weights, lane), lane)


def store_local(out, table, parts, log_weights, lane):
    for h, part in enumerate(parts):
        out[h] = part
    table[...] = table_of(log_weights, lane)


def where_am_i():
    span = lax.axis_index("span")
    return span, 2 * span + lax.axis_index("head") // 2


def unless(seen):
    return jnp.where(seen, 0.0, -jnp.inf)


def first_kernel(queries, key_rows, value_rows, x1, y1, held, sems):
    span, block = where_am_i()
    half = x1.shape[0]
    part = half // 2

    def fetch(array, start, count, slot, place=0):
        source = array.at[:, pl.ds(start, count), :]
        return pltpu.make_async_copy(source, held.at[slot, :, pl.ds(place, count), :], sems.at[slot])

    pairs = (block != 3, span == 0)
    for slot, of_keys in enumerate(pairs):

        @pl.when(of_keys)
        def _():
            fetch(key_rows, slot * half, TILE * 2, slot).start()
            fetch(value_rows, slot * half, TILE * 2, slot, TILE * 2).start()

        @pl.when(jnp.logical_not(of_keys))
        def _():
            fetch(queries, 0, TILE * 4, slot).start()

    for slot, (out, of_keys) in enumerate(zip((x1, y1), pairs)):
        fetch(queries, 0, TILE * 4, slot).wait()

        def turned(start):
            return jnp.swapaxes(held[slot, :, start : start + TILE, :], 0, 1)

        @pl.when(of_keys)
        def _():
            for base, place in ((0, 0), (2 * TILE, part)):
                out[place : place + TILE] = turned(base)
                out[place + TILE : place + part] = turned(base + TILE)[: part - TILE]

        @pl.when(jnp.logical_not(of_keys))
        def _():
            for start in range(0, half, TILE):
                out[start : start + TILE] = turned(start)


def second_kernel(q, k, v, x2, x3, y2, x4):
    span, block = where_am_i()
    part = x2.shape[0]
    half = 2 * part
    taken = x4.shape[0] // 2
    y2[:part] = k[half + part :]
    y2[part:] = v[half + part :]

    @pl.when(span == 0)
    def _():
        x2[...] = k[part:half]
        x3[...] = v[part:half]

    @pl.when(span == 1)
    def _():
        x2[...] = q[half : half + part]
        x3[...] = q[half + part :]

    @pl.when(block == 0)
    def _():
        x4[:taken] = k[2 * half - taken :]
        x4[taken:] = v[2 * half - taken :]

    @pl.when(block != 0)
    def _():
        x4[...] = q[half : half + 2 * taken]


def choose_kernel(x, y, out):
    span, _ = where_am_i()

    @pl.when(span == 0)
    def _():
        out[...] = x[...]

    @pl.when(span == 1)
    def _():
        out[...] = y[...]


def choose_second_kernel(x2, x3, y2, out):
    span, _ = where_am_i()
    part = x2.shape[0]

    @pl.when(span == 0)
    def _():
        out[:part] = x2[...]
        out[part:] = x3[...]

    @pl.when(span == 1)
    def _():
        out[...] = y2[...]


def own_kernel(factor, levels, gate_table, q, k0, k1, v0, v1, out, table, gates):
    span, _ = where_am_i()
    rows, width = q.shape[1:]
    half = out.shape[0]
    heads = [(1 - span) * half + h for h in range(half)]
    jobs = [(q[h], rows_of((k0, h), (k1, h)), rows_of((v0, h), (v1, h))) for h in heads]
    store_local(out, table, *attend(jobs, factor), lanes_of(rows, width))
    level = levels[span]
    lane = lanes_of(1, width)
    for group in range(2):
        row = jnp.zeros((1, width), jnp.float32)
        for h in range(half):
            row = jnp.where(lane == h, gate_table[level, group * half + h], row)
        gates[group : group + 1] = row


def hide(keys, seen_first, seen_second):
    place = lax.broadcasted_iota(jnp.int32, (1, keys), 1)
    return jnp.where(place < keys // 2, unless(seen_first), unless(seen_second))


def visit_kernel(factor, chunk, y1, x, got, got1, k0, k1, v0, v1, out, q):
    span, block = where_am_i()
    part, rows, width = x.shape

    @pl.when(span == 0)
    def _():
        q[...] = y1[chunk * part : (chunk + 1) * part]

    @pl.when(span == 1)
    def _():
        q[...] = x[...]

    jobs = []
    for h in range(part):
        g = (2 * span + chunk) * part + h
        jobs.append(
            (
                q[h],
                rows_of((got, h), (got1, h), (k0, g), (k1, g)),
                rows_of((got, part + h), (got1, part + h), (v0, g), (v1, g)),
            )
        )
    shift = hide(4 * rows, block >= 0, block != 3)
    store(out, *attend(jobs, factor, shift), lanes_of(rows, width))


def stay_kernel(factor, q, a, a1, b, b1, k0, k1, v0, v1, out, table):
    span, block = where_am_i()
    rows, width = q.shape[1:]
    half = out.shape[0]
    part = half // 2
    jobs = []
    for h in range(half):
        g = span * half + h
        first, second = (a, a1) if h < part else (b, b1)
        i = h % part
        jobs.append(
            (
                q[g],
                rows_of((first, i), (second, i), (k0, g), (k1, g)),
                rows_of((first, part + i), (second, part + i), (v0, g), (v1, g)),
            )
        )
    shift = hide(4 * rows, block != 0, block >= 0)
    store_local(out, table, *attend(jobs, factor, shift), lanes_of(rows, width))


def guest_kernel(factor, host, first, skip, q, k0, k1, v0, v1, out):
    _, block = where_am_i()
    heads, rows, width = out.shape[0] - 1, *q.shape[1:]

    @pl.when(block == host)
    def _():
        jobs = [
            (q[skip + h], rows_of((k0, first + h), (k1, first + h)), rows_of((v0, first + h), (v1, first + h)))
            for h in range(heads)
        ]
        store(out, *attend(jobs, factor), lanes_of(rows, width))


def fetched_kernel(factor, host, first, q, got, got1, out, table):
    _, block = where_am_i()
    heads, rows, width = out.shape

    @pl.when(block == host)
    def _():
        jobs = [
            (q[first + h], rows_of((got, h), (got1, h)), rows_of((got, heads + h), (got1, heads + h)))
            for h in range(heads)
        ]
        store_local(out, table, *attend(jobs, factor), lanes_of(rows, width))


def merged(gate_row, logs, parts_of, tiles, first_head, slot, held, out, sems):
    top = functools.reduce(jnp.maximum, logs)
    scaled = [jnp.exp2(table - top) for table in logs]
    ratio = gate_row / sum(scaled)
    scaled = [s * ratio for s in scaled]
    copies = []
    for i, start in enumerate(tile * TILE for tile in tiles):
        sums = [
            sum(part.astype(jnp.float32) * s[:, h : h + 1] for part, s in zip(parts_of(h), scaled))
            for h in range(start, start + TILE)
        ]
        held[slot + i] = jnp.swapaxes(jnp.stack(sums), 0, 1).astype(held.dtype)
        place = out.at[:, pl.ds(first_head + start, TILE), :]
        copies.append(pltpu.make_async_copy(held.at[slot + i], place, sems.at[slot + i]))
        copies[-1].start()
    return copies


def finish(copies):
    for copy in copies:
        copy.wait()


def logs_of(slab):
    return joined(slab[slab.shape[0] - 1])


def side_by_side(first, second, count):
    lane = lanes_of(*first.shape)
    return jnp.where(lane < count, first, pltpu.roll(second, count, 1))


def picked(first, second, h, count):
    return first[h] if h < count else second[h - count]


def merge_first_kernel(
    gates, other, other_table, mine, mine_table, upper, upper2, extra, third, third_table, across, fetched,
    fetched_table, out, held, sems,
):
    _, block = where_am_i()
    half = mine.shape[0]
    part = upper.shape[0] - 1
    lent_heads = half - fetched.shape[0]
    every = range(half // TILE)
    sink = (held, out, sems)

    def visited(more_logs, more_parts):
        logs = [other_table[...], side_by_side(logs_of(upper), logs_of(upper2), part), *more_logs]
        copies = merged(
            gates[0:1],
            logs,
            lambda h: [other[h], picked(upper, upper2, h, part), *more_parts(h)],
            every, 0, 0, *sink,
        )
        logs = [mine_table[...], logs_of(across)]
        early = merged(
            gates[1:2], logs, lambda h: [mine[h], across[h]], every[: part // TILE], half, len(every), *sink
        )
        finish(copies + early)

    @pl.when(block == 2)
    def _():
        visited([], lambda h: [])

    @pl.when(block == 3)
    def _():
        visited(
            [side_by_side(third_table[...], logs_of(extra), part)], lambda h: [picked(third, extra, h, part)]
        )

    @pl.when(block == 0)
    def _():
        copies = merged(gates[0:1], [mine_table[...]], lambda h: [mine[h]], every, 0, 0, *sink)
        early = merged(gates[1:2], [other_table[...]], lambda h: [other[h]], every, half, len(every), *sink)
        finish(copies + early)

    @pl.when(block == 1)
    def _():
        copies = merged(gates[0:1], [mine_table[...]], lambda h: [mine[h]], every, 0, 0, *sink)
        logs = [other_table[...], pltpu.roll(fetched_table[...], lent_heads, 1)]
        early = merged(
            gates[1:2],
            logs,
            lambda h: [other[h], fetched[h - lent_heads]],
            every[-(-lent_heads // TILE) :], half, len(every), *sink,
        )
        finish(copies + early)


def merge_second_kernel(
    gates, other, other_table, mine, mine_table, across, across2, lent, fetched, fetched_table, _, out, held, sems
):
    span, block = where_am_i()
    half = mine.shape[0]
    part = across.shape[0] - 1
    lent_heads = half - fetched.shape[0]
    every = range(half // TILE)
    sink = (held, out, sems)

    @pl.when(span == 1)
    def _():
        logs = [mine_table[...], side_by_side(logs_of(across), logs_of(across2), part)]
        finish(
            merged(
                gates[1:2],
                logs,
                lambda h: [mine[h], picked(across, across2, h, part)],
                every[part // TILE :], half, 0, *sink,
            )
        )

    @pl.when(block == 1)
    def _():
        logs = [other_table[...], side_by_side(logs_of(lent), fetched_table[...], lent_heads)]
        finish(
            merged(
                gates[1:2],
                logs,
                lambda h: [other[h], picked(lent, fetched, h, lent_heads)],
                every[: -(-lent_heads // TILE)], half, 0, *sink,
            )
        )


def run(
    kernel, out_shape, operands, scalars=(), space=pltpu.VMEM, scratch=(), room=8 << 20, out_space=pltpu.VMEM, into=None
):
    in_smem, anywhere = pl.BlockSpec(memory_space=pltpu.SMEM), pl.BlockSpec(memory_space=pl.ANY)
    inputs = [in_smem] * len(scalars) + [pl.BlockSpec(memory_space=space)] * len(operands)
    operands = [*scalars, *operands]
    if into is not None:
        operands.append(into)
        inputs.append(anywhere)
    return pl.pallas_call(
        kernel,
        out_shape=out_shape,
        in_specs=inputs,
        out_specs=jax.tree.map(lambda _: pl.BlockSpec(memory_space=out_space), out_shape),
        scratch_shapes=scratch,
        input_output_aliases={} if into is None else {len(operands) - 1: 0},
        compiler_params=pltpu.CompilerParams(vmem_limit_bytes=room),
        cost_estimate=pl.CostEstimate(flops=2_000_000_000, bytes_accessed=1 << 20, transcendentals=0),
    )(*operands)


def by_block(queries, key_rows, value_rows, noise_levels, gate_table):
    rows, heads, width = queries.shape
    half = heads // 2
    part = half // 2
    lent = half // 2
    per_span = lax.axis_size("head")
    share = per_span // 2
    factor = math.log2(math.e) / math.sqrt(width)
    devices = range(2 * per_span)

    def moved(block, target):
        route = [(p, target(p)) for p in devices if target(p) is not None]
        return lax.ppermute(block, ("span", "head"), route)

    def sideways(p):
        return p ^ share

    def other_span(p):
        return p ^ per_span

    def partner(p):
        return p ^ 1

    def only(numbers, target):
        return lambda p: target(p) if p // share in numbers else None

    def up(p):
        return p + per_span if p < per_span else None

    def blocks(*counts):
        return tuple(jax.ShapeDtypeStruct((n, rows, width), jnp.bfloat16) for n in counts)

    def slab(n):
        return blocks(n + 1)[0]

    def kept(n):
        return (
            jax.ShapeDtypeStruct((n, rows, width), jnp.float32),
            jax.ShapeDtypeStruct((rows, width), jnp.float32),
        )

    def kernel(body, out_shape, *operands, **more):
        return run(body, out_shape, operands, **more)

    x1, y1 = kernel(
        first_kernel,
        blocks(half, half),
        queries,
        key_rows,
        value_rows,
        space=pl.ANY,
        room=ROOM,
        scratch=[pltpu.VMEM((2, rows, 4 * TILE, width), jnp.bfloat16), pltpu.SemaphoreType.DMA((2,))],
    )
    x1, y1, *raw = lax.optimization_barrier((x1, y1, queries, key_rows, value_rows))
    q, k, v = (jnp.transpose(a, (1, 0, 2)) for a in raw)
    x2, x3, y2, x4 = kernel(second_kernel, blocks(part, part, half, 2 * (half - lent)), q, k, v)
    x1 = moved(x1, sideways)
    y1 = moved(y1, other_span)
    own_k, own_v = moved(k, partner), moved(v, partner)
    x2, x3 = moved(x2, sideways), moved(x3, sideways)
    y2 = moved(y2, other_span)
    x4 = moved(x4, only((0, 1), sideways))

    own = (k, own_k, v, own_v)
    *other, gates = kernel(
        functools.partial(own_kernel, factor),
        (*kept(half), jax.ShapeDtypeStruct((2, width), jnp.float32)),
        q,
        *own,
        scalars=(noise_levels, gate_table),
    )
    a = kernel(choose_kernel, blocks(half)[0], x1, y1)
    a1 = moved(a, partner)
    x1_1 = moved(x1, only((3,), partner))
    extra = kernel(functools.partial(guest_kernel, factor, 2, part, part), slab(half - part), x1, *own)
    extra = moved(extra, only((2,), sideways))
    third = kernel(functools.partial(fetched_kernel, factor, 3, 0), kept(part), q, x1, x1_1)

    def visit(chunk, x, got, got1):
        return kernel(
            functools.partial(visit_kernel, factor, chunk),
            slab(part),
            y1,
            x,
            got,
            got1,
            *own,
            scratch=[pltpu.VMEM((part, rows, width), jnp.bfloat16)],
        )

    away = visit(0, x2, a, a1)
    upper, across = moved(away, other_span), moved(away, only((2, 3), sideways))
    b = kernel(choose_second_kernel, blocks(half)[0], x2, x3, y2)
    b1 = moved(b, partner)
    away = visit(1, x3, b, b1)
    upper2, across2 = moved(away, up), moved(away, only((2, 3), sideways))
    helped = kernel(functools.partial(guest_kernel, factor, 0, half, 0), slab(lent), x4, *own)
    helped = moved(helped, only((0,), sideways))
    x4_1 = moved(x4, only((1,), partner))
    mine = kernel(functools.partial(stay_kernel, factor), kept(half), q, a, a1, b, b1, *own)
    fetched = kernel(functools.partial(fetched_kernel, factor, 1, half + lent), kept(half - lent), q, x4, x4_1)
    outcome = jax.ShapeDtypeStruct((rows, heads, width), jnp.bfloat16)
    more = dict(
        out_space=pl.ANY,
        scratch=[pltpu.VMEM((heads // TILE, rows, TILE, width), jnp.bfloat16), pltpu.SemaphoreType.DMA((heads // TILE,))],
    )
    out = kernel(
        merge_first_kernel, outcome, gates, *other, *mine, upper, upper2, extra, *third, across, *fetched, **more
    )
    return kernel(
        merge_second_kernel, outcome, gates, *other, *mine, across, across2, helped, *fetched, into=out, **more
    )


def body(queries, key_rows, value_rows, noise_levels, gate_table):
    rows, heads, _ = queries.shape
    spans, per_span = lax.axis_size("span"), lax.axis_size("head")
    two_by_two = spans == 2 and 2 * rows == BLOCK and per_span * rows == 2 * BLOCK
    if two_by_two and heads == 6 * TILE:
        return by_block(queries, key_rows, value_rows, noise_levels, gate_table)
    return by_head(queries, key_rows, value_rows, noise_levels, gate_table)


def solution(mesh):
    tokens = ("video", "span", "head")
    return jax.shard_map(
        body,
        mesh=mesh,
        in_specs=(
            P(tokens, None, None),
            P(tokens, None, None),
            P(tokens, None, None),
            P("video"),
            P(),
        ),
        out_specs=P(tokens, None, None),
        check_vma=False,
    )
```

```python
import functools
import math

import jax
import jax.numpy as jnp
from jax import lax
from jax.experimental import pallas as pl
from jax.experimental.pallas import tpu as pltpu
from jax.sharding import PartitionSpec as P

BLOCK = 128
LEVELS = 8
ROOM = 211 << 18
TILE = 8
LANES = 32


def from_behind(block, axis, distance):
    devices = range(lax.axis_size(axis))
    route = [(i - distance, i) for i in devices if i - distance in devices]
    return lax.ppermute(block, axis, route)


def gate_rows_for(noise_levels, gate_table):
    one_hot = (jnp.arange(LEVELS, dtype=jnp.int32)[None, :] == noise_levels[:, None]).astype(
        jnp.float32
    )
    return jnp.dot(one_hot, gate_table, precision=lax.Precision.HIGHEST)


def by_head(queries, key_rows, value_rows, noise_levels, gate_table):
    row_count, head_count, head_width = queries.shape
    head_groups = lax.axis_size("head")
    per_group = head_count // head_groups
    chain_len = lax.axis_size("span")
    chain_pos = lax.axis_index("span")
    score_scale = 1.0 / math.sqrt(head_width)
    split_shape = (row_count, head_groups, per_group, head_width)
    query_heads, key_heads, value_heads = (
        lax.all_to_all(
            queries.reshape(split_shape), "head", split_axis=1, concat_axis=0, tiled=True
        ),
        lax.all_to_all(
            key_rows.reshape(split_shape), "head", split_axis=1, concat_axis=0, tiled=True
        ),
        lax.all_to_all(
            value_rows.reshape(split_shape), "head", split_axis=1, concat_axis=0, tiled=True
        ),
    )
    span_len = row_count * head_groups
    query_heads = query_heads.reshape(span_len, per_group, head_width)
    key_heads = key_heads.reshape(span_len, per_group, head_width)
    value_heads = value_heads.reshape(span_len, per_group, head_width)
    own_scores = (
        jnp.einsum("qhd,khd->qhk", query_heads, key_heads, preferred_element_type=jnp.float32)
        * score_scale
    )
    query_block = jnp.arange(span_len, dtype=jnp.int32) // BLOCK
    visible = (query_block[None, :] <= query_block[:, None])[:, None, :]
    own_max = jnp.max(jnp.where(visible, own_scores, -jnp.inf), axis=-1)
    own_weights = jnp.where(visible, jnp.exp(own_scores - own_max[..., None]), 0.0)
    own_totals = jnp.sum(own_weights, axis=-1)
    own_acc = jnp.einsum(
        "qhk,khd->qhd",
        own_weights.astype(jnp.bfloat16),
        value_heads,
        preferred_element_type=jnp.float32,
    )
    running = (own_max, own_totals, own_acc)

    def update(state_now, key_block, value_block):
        row_max, totals, accum = state_now
        scores = (
            jnp.einsum("qhd,khd->qhk", query_heads, key_block, preferred_element_type=jnp.float32)
            * score_scale
        )
        new_max = jnp.maximum(row_max, jnp.max(scores, axis=-1))
        rescale = jnp.exp(row_max - new_max)
        weights = jnp.exp(scores - new_max[..., None])
        totals = totals * rescale + jnp.sum(weights, axis=-1)
        accum = accum * rescale[..., None] + jnp.einsum(
            "qhk,khd->qhd",
            weights.astype(jnp.bfloat16),
            value_block,
            preferred_element_type=jnp.float32,
        )
        return (new_max, totals, accum)

    def advance(state_now, inputs):
        key_block, value_block, span_id = inputs
        useful = (span_id >= 0) & (span_id < chain_pos)
        return (
            lax.cond(
                useful,
                lambda inner: update(inner, key_block, value_block),
                lambda inner: inner,
                state_now,
            ),
            None,
        )

    def relay_turn(turn, loop_state):
        state_now, in_hand = loop_state
        in_hand = from_behind(in_hand, "span", 1)
        state_now, _ = advance(state_now, (in_hand[0], in_hand[1], chain_pos - 1 - turn))
        return (state_now, in_hand)

    running, _ = lax.fori_loop(
        0, chain_len - 1, relay_turn, (running, jnp.stack((key_heads, value_heads)))
    )
    _, totals, accum = running
    gate_rows = gate_rows_for(noise_levels, gate_table)
    gate_row = lax.dynamic_index_in_dim(gate_rows, chain_pos, 0, keepdims=False)
    my_gates = lax.dynamic_slice_in_dim(gate_row, lax.axis_index("head") * per_group, per_group, 0)
    result = (accum / totals[..., None] * my_gates[None, :, None]).astype(jnp.bfloat16)
    returned = lax.all_to_all(
        result.reshape(span_len, 1, per_group, head_width),
        "head",
        split_axis=0,
        concat_axis=1,
        tiled=True,
    )
    return returned.reshape(row_count, head_count, head_width)


def attend(jobs, factor, shift=None):
    scores = [
        lax.dot_general(q, k, (((1,), (1,)), ((), ())), preferred_element_type=jnp.float32)
        for q, k, _ in jobs
    ]
    if shift is not None:
        scores = [s + shift for s in scores]
    tops = [jnp.max(s, axis=1, keepdims=True) for s in scores]
    weights = [jnp.exp2((s - top) * factor) for s, top in zip(scores, tops)]
    totals = [jnp.sum(w, axis=1, keepdims=True) for w in weights]
    sums = [
        lax.dot_general(
            w.astype(jnp.bfloat16), v, (((1,), (0,)), ((), ())), preferred_element_type=jnp.float32
        )
        for w, (_, _, v) in zip(weights, jobs)
    ]
    return (
        [s * (1.0 / t) for s, t in zip(sums, totals)],
        [top * factor + jnp.log2(t) for top, t in zip(tops, totals)],
    )


def lanes_of(rows, width):
    return lax.broadcasted_iota(jnp.int32, (rows, width), 1)


def table_of(columns, lane):
    table = jnp.zeros(lane.shape, jnp.float32)
    for h, column in enumerate(columns):
        table = jnp.where(lane % LANES == h, column, table)
    return table


def split_table(table, lane):
    high = table.astype(jnp.bfloat16).astype(jnp.float32)
    rest = table - high
    middle = rest.astype(jnp.bfloat16).astype(jnp.float32)
    parts = jnp.where(lane < LANES, high, jnp.where(lane < 2 * LANES, middle, rest - middle))
    return jnp.where(lane < 3 * LANES, parts, 0.0).astype(jnp.bfloat16)


def joined(table):
    parts = table.astype(jnp.float32)
    return parts + pltpu.roll(parts, parts.shape[1] - LANES, 1) + pltpu.roll(parts, parts.shape[1] - 2 * LANES, 1)


def rows_of(*blocks):
    return jnp.concatenate([array[head] for array, head in blocks], axis=0)


def store(out, parts, log_weights, lane):
    for h, part in enumerate(parts):
        out[h] = part.astype(out.dtype)
    out[len(parts)] = split_table(table_of(log_weights, lane), lane)


def store_local(out, table, parts, log_weights, lane):
    for h, part in enumerate(parts):
        out[h] = part
    table[...] = table_of(log_weights, lane)


def where_am_i():
    span = lax.axis_index("span")
    return span, 2 * span + lax.axis_index("head") // 2


def unless(seen):
    return jnp.where(seen, 0.0, -jnp.inf)


def first_kernel(queries, key_rows, value_rows, x1, y1, held, sems):
    span, block = where_am_i()
    half = x1.shape[0]
    part = half // 2

    def fetch(array, start, count, slot, place=0):
        source = array.at[:, pl.ds(start, count), :]
        return pltpu.make_async_copy(source, held.at[slot, :, pl.ds(place, count), :], sems.at[slot])

    pairs = (block != 3, span == 0)
    for slot, of_keys in enumerate(pairs):

        @pl.when(of_keys)
        def _():
            fetch(key_rows, slot * half, TILE * 2, slot).start()
            fetch(value_rows, slot * half, TILE * 2, slot, TILE * 2).start()

        @pl.when(jnp.logical_not(of_keys))
        def _():
            fetch(queries, 0, TILE * 4, slot).start()

    for slot, (out, of_keys) in enumerate(zip((x1, y1), pairs)):
        fetch(queries, 0, TILE * 4, slot).wait()

        def turned(start):
            return jnp.swapaxes(held[slot, :, start : start + TILE, :], 0, 1)

        @pl.when(of_keys)
        def _():
            for base, place in ((0, 0), (2 * TILE, part)):
                out[place : place + TILE] = turned(base)
                out[place + TILE : place + part] = turned(base + TILE)[: part - TILE]

        @pl.when(jnp.logical_not(of_keys))
        def _():
            for start in range(0, half, TILE):
                out[start : start + TILE] = turned(start)


def second_kernel(q, k, v, x2, x3, y2, x4):
    span, block = where_am_i()
    part = x2.shape[0]
    half = 2 * part
    taken = x4.shape[0] // 2
    y2[:part] = k[half + part :]
    y2[part:] = v[half + part :]

    @pl.when(span == 0)
    def _():
        x2[...] = k[part:half]
        x3[...] = v[part:half]

    @pl.when(span == 1)
    def _():
        x2[...] = q[half : half + part]
        x3[...] = q[half + part :]

    @pl.when(block == 0)
    def _():
        x4[:taken] = k[2 * half - taken :]
        x4[taken:] = v[2 * half - taken :]

    @pl.when(block != 0)
    def _():
        x4[...] = q[half : half + 2 * taken]


def choose_kernel(x, y, out):
    span, _ = where_am_i()

    @pl.when(span == 0)
    def _():
        out[...] = x[...]

    @pl.when(span == 1)
    def _():
        out[...] = y[...]


def choose_second_kernel(x2, x3, y2, out):
    span, _ = where_am_i()
    part = x2.shape[0]

    @pl.when(span == 0)
    def _():
        out[:part] = x2[...]
        out[part:] = x3[...]

    @pl.when(span == 1)
    def _():
        out[...] = y2[...]


def own_kernel(factor, levels, gate_table, q, k0, k1, v0, v1, out, table, gates):
    span, _ = where_am_i()
    rows, width = q.shape[1:]
    half = out.shape[0]
    heads = [(1 - span) * half + h for h in range(half)]
    jobs = [(q[h], rows_of((k0, h), (k1, h)), rows_of((v0, h), (v1, h))) for h in heads]
    store_local(out, table, *attend(jobs, factor), lanes_of(rows, width))
    level = levels[span]
    lane = lanes_of(1, width)
    for group in range(2):
        row = jnp.zeros((1, width), jnp.float32)
        for h in range(half):
            row = jnp.where(lane == h, gate_table[level, group * half + h], row)
        gates[group : group + 1] = row


def hide(keys, seen_first, seen_second):
    place = lax.broadcasted_iota(jnp.int32, (1, keys), 1)
    return jnp.where(place < keys // 2, unless(seen_first), unless(seen_second))


def visit_kernel(factor, chunk, y1, x, got, got1, k0, k1, v0, v1, out, q):
    span, block = where_am_i()
    part, rows, width = x.shape

    @pl.when(span == 0)
    def _():
        q[...] = y1[chunk * part : (chunk + 1) * part]

    @pl.when(span == 1)
    def _():
        q[...] = x[...]

    jobs = []
    for h in range(part):
        g = (2 * span + chunk) * part + h
        jobs.append(
            (
                q[h],
                rows_of((got, h), (got1, h), (k0, g), (k1, g)),
                rows_of((got, part + h), (got1, part + h), (v0, g), (v1, g)),
            )
        )
    shift = hide(4 * rows, block >= 0, block != 3)
    store(out, *attend(jobs, factor, shift), lanes_of(rows, width))


def stay_kernel(factor, q, a, a1, b, b1, k0, k1, v0, v1, out, table):
    span, block = where_am_i()
    rows, width = q.shape[1:]
    half = out.shape[0]
    part = half // 2
    jobs = []
    for h in range(half):
        g = span * half + h
        first, second = (a, a1) if h < part else (b, b1)
        i = h % part
        jobs.append(
            (
                q[g],
                rows_of((first, i), (second, i), (k0, g), (k1, g)),
                rows_of((first, part + i), (second, part + i), (v0, g), (v1, g)),
            )
        )
    shift = hide(4 * rows, block != 0, block >= 0)
    store_local(out, table, *attend(jobs, factor, shift), lanes_of(rows, width))


def guest_kernel(factor, host, first, skip, q, k0, k1, v0, v1, out):
    _, block = where_am_i()
    heads, rows, width = out.shape[0] - 1, *q.shape[1:]

    @pl.when(block == host)
    def _():
        jobs = [
            (q[skip + h], rows_of((k0, first + h), (k1, first + h)), rows_of((v0, first + h), (v1, first + h)))
            for h in range(heads)
        ]
        store(out, *attend(jobs, factor), lanes_of(rows, width))


def fetched_kernel(factor, host, first, q, got, got1, out, table):
    _, block = where_am_i()
    heads, rows, width = out.shape

    @pl.when(block == host)
    def _():
        jobs = [
            (q[first + h], rows_of((got, h), (got1, h)), rows_of((got, heads + h), (got1, heads + h)))
            for h in range(heads)
        ]
        store_local(out, table, *attend(jobs, factor), lanes_of(rows, width))


def merged(gate_row, logs, parts_of, tiles, slot, held):
    top = functools.reduce(jnp.maximum, logs)
    scaled = [jnp.exp2(table - top) for table in logs]
    ratio = gate_row / sum(scaled)
    scaled = [s * ratio for s in scaled]
    for i, start in enumerate(tile * TILE for tile in tiles):
        sums = [
            sum(part.astype(jnp.float32) * s[:, h : h + 1] for part, s in zip(parts_of(h), scaled))
            for h in range(start, start + TILE)
        ]
        held[slot + i] = jnp.swapaxes(jnp.stack(sums), 0, 1).astype(held.dtype)


def leave(held, slot, tiles, first_head, out, sems, first_sem):
    copies = []
    for i, tile in enumerate(tiles):
        place = out.at[:, pl.ds(first_head + tile * TILE, TILE), :]
        copies.append(pltpu.make_async_copy(held.at[slot + i], place, sems.at[first_sem + i]))
        copies[-1].start()
    return copies


def finish(copies):
    for copy in copies:
        copy.wait()


def logs_of(slab):
    return joined(slab[slab.shape[0] - 1])


def side_by_side(first, second, count):
    lane = lanes_of(*first.shape)
    return jnp.where(lane < count, first, pltpu.roll(second, count, 1))


def picked(first, second, h, count):
    return first[h] if h < count else second[h - count]


def merge_first_kernel(
    gates, other, other_table, mine, mine_table, upper, upper2, extra, third, third_table, across, fetched,
    fetched_table, held,
):
    _, block = where_am_i()
    half = mine.shape[0]
    part = upper.shape[0] - 1
    lent_heads = half - fetched.shape[0]
    every = range(half // TILE)

    def visited(more_logs, more_parts):
        logs = [other_table[...], side_by_side(logs_of(upper), logs_of(upper2), part), *more_logs]
        merged(
            gates[0:1],
            logs,
            lambda h: [other[h], picked(upper, upper2, h, part), *more_parts(h)],
            every, 0, held,
        )
        logs = [mine_table[...], logs_of(across)]
        merged(
            gates[1:2], logs, lambda h: [mine[h], across[h]], every[: part // TILE], len(every), held
        )

    @pl.when(block == 2)
    def _():
        visited([], lambda h: [])

    @pl.when(block == 3)
    def _():
        visited(
            [side_by_side(third_table[...], logs_of(extra), part)], lambda h: [picked(third, extra, h, part)]
        )

    @pl.when(block == 0)
    def _():
        merged(gates[0:1], [mine_table[...]], lambda h: [mine[h]], every, 0, held)
        merged(gates[1:2], [other_table[...]], lambda h: [other[h]], every, len(every), held)

    @pl.when(block == 1)
    def _():
        merged(gates[0:1], [mine_table[...]], lambda h: [mine[h]], every, 0, held)
        logs = [other_table[...], pltpu.roll(fetched_table[...], lent_heads, 1)]
        merged(
            gates[1:2],
            logs,
            lambda h: [other[h], fetched[h - lent_heads]],
            every[-(-lent_heads // TILE) :], len(every), held,
        )


def merge_second_kernel(
    gates, other, other_table, mine, mine_table, across, across2, lent, fetched, fetched_table, early, out, held, sems
):
    span, block = where_am_i()
    half = mine.shape[0]
    part = across.shape[0] - 1
    lent_heads = half - fetched.shape[0]
    every = range(half // TILE)
    count = len(every)

    def out_with(early_tiles, late_tiles, compute):
        copies = leave(early, 0, every, 0, out, sems, 0)
        copies += leave(early, count, early_tiles, half, out, sems, count)
        if late_tiles:
            compute(late_tiles)
            copies += leave(held, 0, late_tiles, half, out, sems, count + len(early_tiles))
        finish(copies)

    @pl.when(block == 0)
    def _():
        out_with(every, every[:0], None)

    @pl.when(span == 1)
    def _():
        def compute(tiles):
            logs = [mine_table[...], side_by_side(logs_of(across), logs_of(across2), part)]
            merged(gates[1:2], logs, lambda h: [mine[h], picked(across, across2, h, part)], tiles, 0, held)

        out_with(every[: part // TILE], every[part // TILE :], compute)

    @pl.when(block == 1)
    def _():
        def compute(tiles):
            logs = [other_table[...], side_by_side(logs_of(lent), fetched_table[...], lent_heads)]
            merged(gates[1:2], logs, lambda h: [other[h], picked(lent, fetched, h, lent_heads)], tiles, 0, held)

        border = -(-lent_heads // TILE)
        out_with(every[border:], every[:border], compute)


def run(
    kernel, out_shape, operands, scalars=(), space=pltpu.VMEM, scratch=(), room=8 << 20, out_space=pltpu.VMEM, into=None
):
    in_smem, anywhere = pl.BlockSpec(memory_space=pltpu.SMEM), pl.BlockSpec(memory_space=pl.ANY)
    inputs = [in_smem] * len(scalars) + [pl.BlockSpec(memory_space=space)] * len(operands)
    operands = [*scalars, *operands]
    if into is not None:
        operands.append(into)
        inputs.append(anywhere)
    return pl.pallas_call(
        kernel,
        out_shape=out_shape,
        in_specs=inputs,
        out_specs=jax.tree.map(lambda _: pl.BlockSpec(memory_space=out_space), out_shape),
        scratch_shapes=scratch,
        input_output_aliases={} if into is None else {len(operands) - 1: 0},
        compiler_params=pltpu.CompilerParams(vmem_limit_bytes=room),
        cost_estimate=pl.CostEstimate(flops=2_000_000_000, bytes_accessed=1 << 20, transcendentals=0),
    )(*operands)


def by_block(queries, key_rows, value_rows, noise_levels, gate_table):
    rows, heads, width = queries.shape
    half = heads // 2
    part = half // 2
    lent = half // 2
    per_span = lax.axis_size("head")
    share = per_span // 2
    factor = math.log2(math.e) / math.sqrt(width)
    devices = range(2 * per_span)

    def moved(block, target):
        route = [(p, target(p)) for p in devices if target(p) is not None]
        return lax.ppermute(block, ("span", "head"), route)

    def sideways(p):
        return p ^ share

    def other_span(p):
        return p ^ per_span

    def partner(p):
        return p ^ 1

    def only(numbers, target):
        return lambda p: target(p) if p // share in numbers else None

    def up(p):
        return p + per_span if p < per_span else None

    def blocks(*counts):
        return tuple(jax.ShapeDtypeStruct((n, rows, width), jnp.bfloat16) for n in counts)

    def slab(n):
        return blocks(n + 1)[0]

    def kept(n):
        return (
            jax.ShapeDtypeStruct((n, rows, width), jnp.float32),
            jax.ShapeDtypeStruct((rows, width), jnp.float32),
        )

    def kernel(body, out_shape, *operands, **more):
        return run(body, out_shape, operands, **more)

    x1, y1 = kernel(
        first_kernel,
        blocks(half, half),
        queries,
        key_rows,
        value_rows,
        space=pl.ANY,
        room=ROOM,
        scratch=[pltpu.VMEM((2, rows, 4 * TILE, width), jnp.bfloat16), pltpu.SemaphoreType.DMA((2,))],
    )
    x1, y1, *raw = lax.optimization_barrier((x1, y1, queries, key_rows, value_rows))
    q, k, v = (jnp.transpose(a, (1, 0, 2)) for a in raw)
    x2, x3, y2, x4 = kernel(second_kernel, blocks(part, part, half, 2 * (half - lent)), q, k, v)
    x1 = moved(x1, sideways)
    y1 = moved(y1, other_span)
    own_k, own_v = moved(k, partner), moved(v, partner)
    x2, x3 = moved(x2, sideways), moved(x3, sideways)
    y2 = moved(y2, up)
    x4 = moved(x4, only((0, 1), sideways))

    own = (k, own_k, v, own_v)
    *other, gates = kernel(
        functools.partial(own_kernel, factor),
        (*kept(half), jax.ShapeDtypeStruct((2, width), jnp.float32)),
        q,
        *own,
        scalars=(noise_levels, gate_table),
    )
    a = kernel(choose_kernel, blocks(half)[0], x1, y1)
    a1 = moved(a, partner)
    x1_1 = moved(x1, only((3,), partner))
    extra = kernel(functools.partial(guest_kernel, factor, 2, part, part), slab(half - part), x1, *own)
    extra = moved(extra, only((2,), sideways))
    third = kernel(functools.partial(fetched_kernel, factor, 3, 0), kept(part), q, x1, x1_1)

    def visit(chunk, x, got, got1):
        return kernel(
            functools.partial(visit_kernel, factor, chunk),
            slab(part),
            y1,
            x,
            got,
            got1,
            *own,
            scratch=[pltpu.VMEM((part, rows, width), jnp.bfloat16)],
        )

    away = visit(0, x2, a, a1)
    upper, across = moved(away, other_span), moved(away, only((2, 3), sideways))
    b = kernel(choose_second_kernel, blocks(half)[0], x2, x3, y2)
    b1 = moved(b, partner)
    away = visit(1, x3, b, b1)
    upper2, across2 = moved(away, up), moved(away, only((2, 3), sideways))
    helped = kernel(functools.partial(guest_kernel, factor, 0, half, 0), slab(lent), x4, *own)
    helped = moved(helped, only((0,), sideways))
    x4_1 = moved(x4, only((1,), partner))
    mine = kernel(functools.partial(stay_kernel, factor), kept(half), q, a, a1, b, b1, *own)
    fetched = kernel(functools.partial(fetched_kernel, factor, 1, half + lent), kept(half - lent), q, x4, x4_1)
    tiles = heads // TILE
    early = kernel(
        merge_first_kernel,
        jax.ShapeDtypeStruct((tiles, rows, TILE, width), jnp.bfloat16),
        gates, *other, *mine, upper, upper2, extra, *third, across, *fetched,
    )
    return kernel(
        merge_second_kernel,
        jax.ShapeDtypeStruct((rows, heads, width), jnp.bfloat16),
        gates, *other, *mine, across, across2, helped, *fetched, early,
        out_space=pl.ANY,
        scratch=[pltpu.VMEM((half // TILE, rows, TILE, width), jnp.bfloat16), pltpu.SemaphoreType.DMA((tiles,))],
    )


def body(queries, key_rows, value_rows, noise_levels, gate_table):
    rows, heads, _ = queries.shape
    spans, per_span = lax.axis_size("span"), lax.axis_size("head")
    two_by_two = spans == 2 and 2 * rows == BLOCK and per_span * rows == 2 * BLOCK
    if two_by_two and heads == 6 * TILE:
        return by_block(queries, key_rows, value_rows, noise_levels, gate_table)
    return by_head(queries, key_rows, value_rows, noise_levels, gate_table)


def solution(mesh):
    tokens = ("video", "span", "head")
    return jax.shard_map(
        body,
        mesh=mesh,
        in_specs=(
            P(tokens, None, None),
            P(tokens, None, None),
            P(tokens, None, None),
            P("video"),
            P(),
        ),
        out_specs=P(tokens, None, None),
        check_vma=False,
    )
```
